8 devices in a mesh: sys: 1 (over z), aux: 2 (over y), orb: 4 (over x, core).
Axes of the slice: x: 2, y: 2, z: 1, core: 2. Of those that a mesh axis runs over, the one named last changes fastest.
Arguments:
- aux_ints: float32 [672, 192, 192], P(('sys', 'aux'), 'orb')
- metric: float32 [672, 672], P(('sys', 'aux'))
- orbitals: float32 [4, 192, 40], P('sys')
Outputs:
- output: float32 [4, 192, 192], P('sys', 'orb', 'aux')
All inputs are finite; a program needn't handle non-finite values.
Results may differ from the reference program's by a relative error of at most 0.001.
Values are sent between devices in bfloat16 or wider.
A program may use at most 1 GiB of HBM per device.

```python
import jax
import jax.numpy as jnp
from jax import lax

N_AUX = 672
N_BASIS = 192
N_OCC = 40
DENS = 4

PRECISE = lax.Precision.HIGHEST


def setup_inputs(seed: int = 0, part: int = 0) -> dict:
    base_key = jax.random.fold_in(jax.random.key(seed), part)
    sub_keys = jax.random.split(base_key, 6)
    rank_b = 4
    rank_m = 4
    coh_scale = (2.0 * N_AUX * N_OCC) ** -0.5 * rank_b ** -0.25
    noise_scale = 2.0 * coh_scale
    coeffs = jax.random.normal(sub_keys[0], (N_AUX, rank_b), jnp.float32)
    patterns = jax.random.normal(sub_keys[1], (rank_b, N_BASIS), jnp.float32)
    row_keys = jax.random.split(sub_keys[2], N_AUX)

    def one_row(row_args):
        row_key, coeff_row = row_args
        noise_mat = jax.random.normal(row_key, (N_BASIS, N_BASIS), jnp.float32)
        sym_noise = (noise_mat + noise_mat.T) * (0.5 ** 0.5)
        low_rank = jnp.einsum('k,km,kl->ml', coeff_row, patterns, patterns)
        return noise_scale * sym_noise + coh_scale * low_rank

    aux_ints = lax.map(one_row, (row_keys, coeffs))
    spread = jax.random.normal(sub_keys[3], (N_AUX, N_AUX), jnp.float32)
    sym_spread = (spread + spread.T) * (0.125 / N_AUX) ** 0.5
    directions = jax.random.normal(sub_keys[4], (rank_m, N_AUX), jnp.float32) * N_AUX ** -0.5
    boost_scale = (N_AUX / rank_m) ** 0.5
    metric = jnp.eye(N_AUX, dtype=jnp.float32) + sym_spread + boost_scale * jnp.dot(directions.T, directions)
    orbitals = jax.random.normal(sub_keys[5], (DENS, N_BASIS, N_OCC), jnp.float32) * N_BASIS ** -0.5
    return {'aux_ints': aux_ints, 'metric': metric, 'orbitals': orbitals}


def reference(aux_ints, metric, orbitals):
    def one_density(coeff_mat):
        half_tr = jnp.einsum('qml,li->qmi', aux_ints, coeff_mat, precision=PRECISE)
        fitted = jnp.einsum('pq,qmi->pmi', metric, half_tr, precision=PRECISE)
        exchange = jnp.einsum('pmi,pni->mn', fitted, fitted, precision=PRECISE)
        gamma_raw = jnp.einsum('qmi,mi->q', half_tr, coeff_mat, precision=PRECISE)
        gamma_fit = jnp.dot(metric, gamma_raw, precision=PRECISE)
        weights = jnp.dot(gamma_fit, metric, precision=PRECISE)
        coulomb = jnp.einsum('q,qmn->mn', weights, aux_ints, precision=PRECISE)
        return 2.0 * coulomb - exchange

    return lax.map(one_density, orbitals)
```

```python
import functools

import jax
import jax.numpy as jnp
from jax import lax
from jax.experimental import pallas as pl
from jax.experimental.pallas import tpu as pltpu
from jax.sharding import PartitionSpec as P

MESH = pl.DeviceIdType.MESH
F32, BF16 = jnp.float32, jnp.bfloat16
HIGHEST = lax.Precision.HIGHEST

DENS, L, OCC = 4, 192, 40
COLS = DENS * OCC
MINE = COLS // 8
ROWS = 48
GROUP = 16
GROUPS = ROWS // GROUP
QL, QP = 336, 384
TAIL = QL - 256
STRIDE = 168
NT = (((1,), (1,)), ((), ()))


def _subsets(sizes):
    out, first, off = [], 0, 0
    for n in sizes:
        tails = 2 * (n // 3) + n % 3
        out.append((first, n, off, 2 * n + tails))
        first, off = first + n, off + 2 * n + tails
    return out, off


SUBSETS, SLOTS = _subsets((8, 8, 4))
MAXSUB = max(s[1] for s in SUBSETS)


def _split(v):
    one = v.astype(BF16)
    rest = v - one.astype(F32)
    two = rest.astype(BF16)
    return one, two, (rest - two.astype(F32)).astype(BF16)


def _dot(p, q):
    return jnp.dot(p, q, preferred_element_type=F32)


def _dot_nt(p, q):
    return lax.dot_general(p, q, NT, preferred_element_type=F32)


def _padq(v):
    return jnp.pad(v, ((0, 0), (0, QP - QL)))


def kernel(b_hbm, ct_ref, met_ref, out_ref,
           b_ref, c_ref, dfull, dm_ref, s_ref, snd, rcv, hl, m_ref, mx, mr, t_ref,
           ga_ref, gr_ref, j_ref, jown, jsend, jrecv, kacc, xacc, ksend, krecv,
           bsem, hs_sem, hr_sem, ms_sem, mr_sem, gs_sem, gr_sem, js_sem, jr_sem, ks_sem, kr_sem):
    a = lax.axis_index('aux')
    o = lax.axis_index('orb')
    x, c = o // 2, o % 2
    sys = lax.axis_index('sys')

    def peer(k):
        return (a + k // 4) % 2, (x + (k // 2) % 2) % 2, (c + k % 2) % 2

    def device(k):
        pa, px, pc = peer(k)
        return (sys, pa, px * 2 + pc)

    def remote(src, dst, ssem, rsem, k):
        return pltpu.make_async_remote_copy(src_ref=src, dst_ref=dst, send_sem=ssem, recv_sem=rsem,
                                            device_id=device(k), device_id_type=MESH)

    def b_copy(g):
        return pltpu.make_async_copy(b_hbm.at[pl.ds(g * GROUP, GROUP)], b_ref.at[pl.ds(g * GROUP, GROUP)], bsem.at[g])

    def h_copy(k, g, s):
        _, _, off, n = SUBSETS[s]
        return remote(snd.at[k - 1, g, pl.ds(off, n)], rcv.at[k, g, pl.ds(off, n)],
                      hs_sem.at[k, g, s], hr_sem.at[k, g, s], k)

    ORDER = (2, 4, 6, 3, 5, 7, 1)

    def h_send(g, s):
        for k in ORDER:
            h_copy(k, g, s).start()

    def m_copy(step):
        rows = pl.ds(pl.multiple_of(c * (QL // 2), 8), QL // 2)
        return remote((mx if step == 0 else mr).at[rows], mr.at[rows], ms_sem.at[step], mr_sem.at[step], 4 if step == 0 else 1)

    def g_copy(k):
        return remote(ga_ref, gr_ref.at[k], gs_sem.at[k], gr_sem.at[k], k)

    def j_copy():
        return remote(jsend, jrecv, js_sem, jr_sem, 4)

    def k_copy(k):
        return remote(ksend.at[k], krecv.at[k], ks_sem.at[k], kr_sem.at[k], k)

    for g in range(GROUPS):
        b_copy(g).start()

    barrier = pltpu.get_barrier_semaphore()
    for k in range(1, 8):
        pl.semaphore_signal(barrier, inc=1, device_id=device(k), device_id_type=MESH)

    met = met_ref[...]
    low, high = _padq(met[:, :QL]), _padq(met[:, QL:])
    own = jnp.where(a == 0, low, high)
    oth = jnp.where(a == 0, high, low)
    mx[...] = own

    def m_store(block, row, col):
        for j, term in enumerate(_split(block)):
            m_ref[pl.ds(j * 2 * QP + row, block.shape[0]), pl.ds(col, QP)] = term

    m_store(oth, 0, QP)
    m_store(jnp.pad(oth, ((0, QP - QL), (0, 0))).T, QP, 0)
    m_store(own, 0, 0)
    for j in range(3):
        m_ref[pl.ds(j * 2 * QP + QL, QP - QL), :] = jnp.zeros((QP - QL, 2 * QP), BF16)
        m_ref[pl.ds(j * 2 * QP + QP + QL, QP - QL), pl.ds(QP, QP)] = jnp.zeros((QP - QL, QP), BF16)
    pl.semaphore_wait(barrier, 7)
    m_copy(0).start()

    for j, term in enumerate(_split(ct_ref[...])):
        c_ref[j] = term
    dm_ref[...] = jnp.zeros_like(dm_ref)
    for d in range(DENS):
        cd = ct_ref[pl.ds(d * OCC, OCC), :]
        dfull[...] = lax.dot_general(cd, cd, (((0,), (0,)), ((), ())), precision=HIGHEST, preferred_element_type=F32)
        dm_ref[:, d, :] = dfull[pl.ds(pl.multiple_of(o * ROWS, 8), ROWS), :]

    lane = lax.broadcasted_iota(jnp.int32, (GROUP, 128), 1)

    def half_transform(g):
        def body(p, ga):
            m = g * GROUP + 2 * p
            b1, b2, b3 = _split(jnp.concatenate([_padq(b_ref[m]), _padq(b_ref[m + 1])], axis=1))
            d1, d2, d3 = _split(dm_ref[pl.ds(m, 2)].reshape(16, L))
            lhs = jnp.concatenate([c_ref[0], d1, c_ref[1], d2, c_ref[2], d3], axis=0)
            n = COLS + 16
            r1, r2, r3 = _dot(lhs, b1), _dot(lhs[:2 * n], b2), _dot(lhs[:n], b3)
            h = r1[:n] + ((r1[n:2 * n] + r2[:n]) + (r1[2 * n:] + (r2[n:] + r3)))
            for q in range(2):
                for t in range(3):
                    s_ref[t, pl.ds(pl.multiple_of((2 * p + q) * STRIDE, 8), COLS), :] = h[:COLS, q * QP + t * 128:q * QP + (t + 1) * 128]
            return ga + h[COLS:COLS + 8, :QP] + h[COLS + 8:, QP:]

        ga_ref[...] = lax.fori_loop(0, GROUP // 2, body, jnp.zeros((8, QP), F32) if g == 0 else ga_ref[...])

    def pack(k, g, dst):
        pa, px, pc = peer(k)
        first = (pa * 4 + px * 2 + pc) * MINE

        def load(t, i):
            return s_ref[t, pl.ds(first + i, GROUP, stride=STRIDE), :]

        for i0, n, off, _ in SUBSETS:
            for i in range(n):
                dst[off + i] = load(0, i0 + i).astype(BF16)
                dst[off + n + i] = load(1, i0 + i).astype(BF16)
            at = off + 2 * n
            for j in range(n // 3):
                third = load(2, i0 + 3 * j + 2)
                dst[at + 2 * j] = jnp.where(lane < TAIL, load(2, i0 + 3 * j), pltpu.roll(third, TAIL, 1)).astype(BF16)
                dst[at + 2 * j + 1] = jnp.where(lane < TAIL, load(2, i0 + 3 * j + 1), pltpu.roll(third, 32, 1)).astype(BF16)
            for i in range(n - n % 3, n):
                dst[at + 2 * (n // 3) + i - (n - n % 3)] = load(2, i0 + i).astype(BF16)

    def pack_all(g):
        def body(k, carry):
            pack(k, g, snd.at[k - 1, g])
            return carry

        lax.fori_loop(1, 8, body, 0)
        pack(0, g, rcv.at[0, g])
        first = (a * 4 + x * 2 + c) * MINE
        for i in range(MINE):
            for t in range(3):
                _, two, three = _split(s_ref[t, pl.ds(first + i, GROUP, stride=STRIDE), :])
                hl[0, g, i, :, pl.ds(t * 128, 128)] = two
                hl[1, g, i, :, pl.ds(t * 128, 128)] = three

    b_copy(0).wait()
    half_transform(0)
    pack_all(0)
    h_send(0, 0)
    b_copy(1).wait()
    half_transform(1)
    pack_all(1)
    m_copy(0).wait_recv()
    m_copy(1).start()
    b_copy(2).wait()
    half_transform(2)
    for k in (1, 2, 3, 4, 5, 6, 7):
        g_copy(k).start()
    h_send(1, 0)
    pack_all(2)
    h_send(2, 0)
    for g in range(GROUPS):
        h_send(g, 1)

    m_copy(1).wait_recv()
    m_store(mr[...], QP, QP)

    for k in range(1, 8):
        g_copy(k).wait_recv()
    gam = jnp.concatenate([ga_ref[...] + gr_ref[1] + gr_ref[2] + gr_ref[3],
                           gr_ref[4] + gr_ref[5] + gr_ref[6] + gr_ref[7]], axis=1)

    def stack(v):
        return jnp.concatenate([t.astype(F32) for t in _split(v)], axis=0).astype(BF16)

    def three(v, dot):
        r1, r2, r3 = dot(v, 0), dot(v[:16], 1), dot(v[:8], 2)
        return r1[:8] + ((r1[8:16] + r2[:8]) + (r1[16:] + (r2[8:] + r3)))

    fit = three(stack(gam), lambda v, j: _dot(v, m_ref[pl.ds(j * 2 * QP, 2 * QP), :]))
    weights = three(stack(fit), lambda v, j: _dot(v, m_ref[pl.ds(j * 2 * QP, 2 * QP), pl.ds(0, QP)]))
    wstack = stack(weights)

    def coulomb(m, carry):
        terms = _split(_padq(b_ref[m]))
        j_ref[m] = three(wstack, lambda v, j: _dot_nt(v, terms[j]))
        return carry

    lax.fori_loop(0, ROWS, coulomb, 0)
    for d in range(DENS):
        jd = j_ref[:, d, :]
        jown[d] = jnp.where(a == 0, jd[:, :96], jd[:, 96:])
        jsend[d] = jnp.where(a == 0, jd[:, 96:], jd[:, :96])
    j_copy().start()

    kacc[...] = jnp.zeros_like(kacc)
    xacc[...] = jnp.zeros_like(xacc)

    for s, (i0, n, off, _) in enumerate(SUBSETS):
        if s == 1:
            for g in range(GROUPS):
                h_send(g, 2)

        def half(k, g):
            first = rcv[k, g, pl.ds(off, n)].reshape(n * GROUP, 128)
            second = rcv[k, g, pl.ds(off + n, n)].reshape(n * GROUP, 128)
            at, tails = off + 2 * n, []
            for j in range(n // 3):
                p, q = rcv[k, g, at + 2 * j], rcv[k, g, at + 2 * j + 1]
                third = jnp.where(lane < 128 - TAIL, pltpu.roll(p.astype(F32), 128 - TAIL, 1), pltpu.roll(q.astype(F32), 96, 1))
                tails += [p, q, third.astype(BF16)]
            for i in range(n % 3):
                tails.append(rcv[k, g, at + 2 * (n // 3) + i])
            return jnp.concatenate([first, second, jnp.concatenate(tails, axis=0)], axis=1)

        def fit_group(g, carry):
            for k in range(1, 8):
                h_copy(k, g, s).wait_recv()
            lhs = jnp.concatenate([jnp.concatenate([half(k, g), half(k + 4, g)], axis=1) for k in range(4)], axis=0)
            t = _dot(jnp.concatenate([lhs, lhs, lhs], axis=1), m_ref[...])
            h2 = hl[0, g, pl.ds(i0, n)].reshape(n * GROUP, QP)
            h3 = hl[1, g, pl.ds(i0, n)].reshape(n * GROUP, QP)
            ca = _dot(jnp.concatenate([h2, h3], axis=0), m_ref[pl.ds(0, QP), :])
            cb = _dot(h2, m_ref[pl.ds(2 * QP, QP), :])
            w = n * GROUP
            for k in range(4):
                _, px, pc = peer(k)
                part = t[k * w:(k + 1) * w]
                if k == 0:
                    part = part + (ca[:w] + (ca[w:] + cb))
                row = pl.multiple_of((px * 2 + pc) * ROWS + g * GROUP, GROUP)
                t_ref[pl.ds(0, n), pl.ds(row, GROUP), :] = part.reshape(n, GROUP, 2 * QP)
            return carry

        lax.fori_loop(0, GROUPS, fit_group, 0)

        def exchange(i, carry):
            t1, t2, t3 = _split(t_ref[i])
            one = jnp.concatenate([t1, t2], axis=1)
            kacc[...] += _dot_nt(one, one)
            xacc[...] += _dot_nt(jnp.concatenate([t1, t1], axis=1), jnp.concatenate([t2, t3], axis=1))
            return carry

        lax.fori_loop(0, n, exchange, 0)

    kacc[...] += xacc[...] + xacc[...].T
    for k in (7, 6, 5, 4, 3, 2, 1, 0):
        pa, px, pc = peer(k)
        rows = kacc[pl.ds(pl.multiple_of((px * 2 + pc) * ROWS, 8), ROWS), :]
        part = jnp.where(pa == 0, rows[:, :96], rows[:, 96:])
        if k:
            ksend[k] = part
        else:
            krecv[0] = part
    for k in (7, 6, 5, 4, 3, 2, 1):
        k_copy(k).start()
    j_copy().wait_recv()
    for k in range(1, 8):
        k_copy(k).wait_recv()
    for k in (0, 2, 4, 6):
        pa, px, _ = peer(k)
        d = pa * 2 + px
        out_ref[d] = 2.0 * (jown[d] + jrecv[d]) - (krecv[k] + krecv[k + 1])

    for k in range(1, 8):
        for g in range(GROUPS):
            for s in range(len(SUBSETS)):
                h_copy(k, g, s).wait_send()
        g_copy(k).wait_send()
        k_copy(k).wait_send()
    m_copy(0).wait_send()
    m_copy(1).wait_send()
    j_copy().wait_send()


def solution(mesh):
    def local_fock(ints_blk, metric_blk, orbitals):
        bt = jnp.transpose(ints_blk, (1, 2, 0))
        ct = jnp.transpose(orbitals, (0, 2, 1)).reshape(COLS, L)
        ns = len(SUBSETS)
        dma = pltpu.SemaphoreType.DMA
        return pl.pallas_call(
            kernel,
            out_shape=jax.ShapeDtypeStruct((DENS, ROWS, 96), F32),
            in_specs=[pl.BlockSpec(memory_space=pl.ANY), pl.BlockSpec(memory_space=pltpu.VMEM), pl.BlockSpec(memory_space=pltpu.VMEM)],
            out_specs=pl.BlockSpec(memory_space=pltpu.VMEM),
            scratch_shapes=[
                pltpu.VMEM((ROWS, L, QL), F32),
                pltpu.VMEM((3, COLS, L), BF16),
                pltpu.VMEM((L, L), F32),
                pltpu.VMEM((ROWS, 8, L), F32),
                pltpu.VMEM((3, GROUP * STRIDE, 128), F32),
                pltpu.VMEM((7, GROUPS, SLOTS, GROUP, 128), BF16),
                pltpu.VMEM((8, GROUPS, SLOTS, GROUP, 128), BF16),
                pltpu.VMEM((2, GROUPS, MINE, GROUP, QP), BF16),
                pltpu.VMEM((6 * QP, 2 * QP), BF16),
                pltpu.VMEM((QL, QP), F32),
                pltpu.VMEM((QL, QP), F32),
                pltpu.VMEM((MAXSUB, L, 2 * QP), F32),
                pltpu.VMEM((8, QP), F32),
                pltpu.VMEM((8, 8, QP), F32),
                pltpu.VMEM((ROWS, 8, L), F32),
                pltpu.VMEM((DENS, ROWS, 96), F32),
                pltpu.VMEM((DENS, ROWS, 96), F32),
                pltpu.VMEM((DENS, ROWS, 96), F32),
                pltpu.VMEM((L, L), F32),
                pltpu.VMEM((L, L), F32),
                pltpu.VMEM((8, ROWS, 96), F32),
                pltpu.VMEM((8, ROWS, 96), F32),
                dma((GROUPS,)), dma((8, GROUPS, ns)), dma((8, GROUPS, ns)), dma((2,)), dma((2,)),
                dma((8,)), dma((8,)), dma, dma, dma((8,)), dma((8,)),
            ],
            compiler_params=pltpu.CompilerParams(collective_id=0, has_side_effects=True, vmem_limit_bytes=60 * 1024 * 1024),
            cost_estimate=pl.CostEstimate(flops=25_000_000_000, bytes_accessed=16_000_000, transcendentals=0),
        )(bt, ct, metric_blk)

    return jax.shard_map(local_fock, mesh=mesh, in_specs=(P(('sys', 'aux'), 'orb', None), P(('sys', 'aux'), None), P('sys', None, None)), out_specs=P('sys', 'orb', 'aux'), check_vma=False)
```

```python
import functools

import jax
import jax.numpy as jnp
from jax import lax
from jax.experimental import pallas as pl
from jax.experimental.pallas import tpu as pltpu
from jax.sharding import PartitionSpec as P

MESH = pl.DeviceIdType.MESH
F32, BF16 = jnp.float32, jnp.bfloat16
HIGHEST = lax.Precision.HIGHEST

DENS, L, OCC = 4, 192, 40
COLS = DENS * OCC
MINE = COLS // 8
ROWS = 48
GROUP = 16
GROUPS = ROWS // GROUP
QL, QP = 336, 384
TAIL = QL - 256
STRIDE = 168
HALFC = COLS // 2
MQ = 88
WPAD = 32
NT = (((1,), (1,)), ((), ()))


def _subsets(sizes):
    out, first, off = [], 0, 0
    for n in sizes:
        tails = 2 * (n // 3) + n % 3
        out.append((first, n, off, 2 * n + tails))
        first, off = first + n, off + 2 * n + tails
    return out, off


SUBSETS, SLOTS = _subsets((9, 6, 3, 2))
MAXSUB = max(s[1] for s in SUBSETS)


def _split(v):
    one = v.astype(BF16)
    rest = v - one.astype(F32)
    two = rest.astype(BF16)
    return one, two, (rest - two.astype(F32)).astype(BF16)


def _dot(p, q):
    return jnp.dot(p, q, preferred_element_type=F32)


def _dot_nt(p, q):
    return lax.dot_general(p, q, NT, preferred_element_type=F32)


def _padq(v):
    return jnp.pad(v, ((0, 0), (0, QP - QL)))


def kernel(b_hbm, ct_hbm, met_hbm, out_ref,
           b_ref, ct_ref, met_ref, c_ref, ctt, dm_ref, s_ref, snd, rcv, hl, m_ref, mx, mr, t_ref, w_ref,
           ga_ref, gr_ref, j_ref, jown, jsend, jrecv, kacc, xacc, ksend, krecv,
           bsem, isem, hs_sem, hr_sem, ms_sem, mr_sem, gs_sem, gr_sem, js_sem, jr_sem, ks_sem, kr_sem):
    a = lax.axis_index('aux')
    o = lax.axis_index('orb')
    x, c = o // 2, o % 2
    sys = lax.axis_index('sys')

    def peer(k):
        return (a + k // 4) % 2, (x + (k // 2) % 2) % 2, (c + k % 2) % 2

    def device(k):
        pa, px, pc = peer(k)
        return (sys, pa, px * 2 + pc)

    def remote(src, dst, ssem, rsem, k):
        return pltpu.make_async_remote_copy(src_ref=src, dst_ref=dst, send_sem=ssem, recv_sem=rsem,
                                            device_id=device(k), device_id_type=MESH)

    def b_copy(j):
        return pltpu.make_async_copy(b_hbm.at[pl.ds(j * 8, 8)], b_ref.at[pl.ds(j * 8, 8)], bsem.at[j])

    def h_copy(k, g, s):
        _, _, off, n = SUBSETS[s]
        return remote(snd.at[k - 1, g, pl.ds(off, n)], rcv.at[k, g, pl.ds(off, n)],
                      hs_sem.at[k, g, s], hr_sem.at[k, g, s], k)

    FAR, NEAR = (4, 6, 5, 7), (2, 3, 1)

    def h_send(g, s, ks=(4, 6, 2, 5, 7, 3, 1)):
        for k in ks:
            h_copy(k, g, s).start()

    def m_copy(step):
        mine = o if step < 3 else (1 - x) * 2 + c
        src = mx.at[pl.ds(pl.multiple_of(o * MQ - (o // 3) * (4 * MQ - QL), 8), MQ)] if step == 0 else mr.at[mine]
        return remote(src, mr.at[mine], ms_sem.at[step], mr_sem.at[step], (4, 2, 1, 1)[step])

    def g_copy(k):
        return remote(ga_ref, gr_ref.at[k], gs_sem.at[k], gr_sem.at[k], k)

    def j_copy():
        return remote(jsend, jrecv, js_sem, jr_sem, 4)

    def k_copy(k):
        return remote(ksend.at[k], krecv.at[k], ks_sem.at[k], kr_sem.at[k], k)

    ct_copy = pltpu.make_async_copy(ct_hbm, ct_ref, isem.at[0])
    met_copy = pltpu.make_async_copy(met_hbm, met_ref, isem.at[1])
    ct_copy.start()
    met_copy.start()
    for j in range(ROWS // 8):
        b_copy(j).start()

    barrier = pltpu.get_barrier_semaphore()
    for k in range(1, 8):
        pl.semaphore_signal(barrier, inc=1, device_id=device(k), device_id_type=MESH)

    ct_copy.wait()
    for j, term in enumerate(_split(ct_ref[...])):
        c_ref[j] = term

    met_copy.wait()
    met = met_ref[...]
    low, high = _padq(met[:, :QL]), _padq(met[:, QL:])
    own = jnp.where(a == 0, low, high)
    mx[...] = own
    pl.semaphore_wait(barrier, 7)

    def m_store(block, row, col):
        for j, term in enumerate(_split(block)):
            m_ref[pl.ds(j * 2 * QP + row, block.shape[0]), pl.ds(col, QP)] = term

    lane = lax.broadcasted_iota(jnp.int32, (GROUP, 128), 1)

    def density_rows():
        ctt[...] = ct_ref[...].T
        rows = ctt[pl.ds(pl.multiple_of(o * ROWS, 8), ROWS), :]
        col = lax.broadcasted_iota(jnp.int32, (ROWS, COLS), 1)
        masked = [jnp.where((col >= d * OCC) & (col < (d + 1) * OCC), rows, 0.0) for d in range(DENS)]
        dens = jnp.dot(jnp.concatenate(masked, axis=0), ct_ref[...], precision=HIGHEST, preferred_element_type=F32)
        dm_ref[...] = jnp.zeros_like(dm_ref)
        for d in range(DENS):
            dm_ref[:, d, :] = dens[d * ROWS:(d + 1) * ROWS]

    def half_transform(g, start, n, with_gamma):
        def body(p, ga):
            m = g * GROUP + 2 * p
            b1, b2, b3 = _split(jnp.concatenate([_padq(b_ref[m]), _padq(b_ref[m + 1])], axis=1))
            terms = [c_ref[j, pl.ds(start, n), :] for j in range(3)]
            if with_gamma:
                extra = _split(dm_ref[pl.ds(m, 2)].reshape(16, L))
                terms = [jnp.concatenate(pair, axis=0) for pair in zip(terms, extra)]
            w = terms[0].shape[0]
            lhs = jnp.concatenate(terms, axis=0)
            r1, r2, r3 = _dot(lhs, b1), _dot(lhs[:2 * w], b2), _dot(lhs[:w], b3)
            h = r1[:w] + ((r1[w:2 * w] + r2[:w]) + (r1[2 * w:] + (r2[w:] + r3)))
            for q in range(2):
                row = pl.multiple_of((2 * p + q) * STRIDE + start, 8)
                for t in range(3):
                    s_ref[t, pl.ds(row, n), :] = h[:n, q * QP + t * 128:q * QP + (t + 1) * 128]
            if with_gamma:
                ga = ga + h[n:n + 8, :QP] + h[n + 8:, QP:]
            return ga

        return body

    def run_half(g, start, n, with_gamma, waits):
        body = half_transform(g, start, n, with_gamma)
        ga = (jnp.zeros((8, QP), F32) if g == 0 else ga_ref[...]) if with_gamma else 0
        for j in range(2):
            if waits:
                b_copy(2 * g + j).wait()
            ga = lax.fori_loop(4 * j, 4 * j + 4, body, ga)
        if with_gamma:
            ga_ref[...] = ga

    def pack(k, g, dst):
        pa, px, pc = peer(k)
        first = (pa * 4 + px * 2 + pc) * MINE

        def load(t, i):
            return s_ref[t, pl.ds(first + i, GROUP, stride=STRIDE), :]

        for i0, n, off, _ in SUBSETS:
            for i in range(n):
                dst[off + i] = load(0, i0 + i).astype(BF16)
                dst[off + n + i] = load(1, i0 + i).astype(BF16)
            at = off + 2 * n
            for j in range(n // 3):
                third = load(2, i0 + 3 * j + 2)
                dst[at + 2 * j] = jnp.where(lane < TAIL, load(2, i0 + 3 * j), pltpu.roll(third, TAIL, 1)).astype(BF16)
                dst[at + 2 * j + 1] = jnp.where(lane < TAIL, load(2, i0 + 3 * j + 1), pltpu.roll(third, 32, 1)).astype(BF16)
            for i in range(n - n % 3, n):
                dst[at + 2 * (n // 3) + i - (n - n % 3)] = load(2, i0 + i).astype(BF16)

    def pack_range(g, k0, k1):
        def body(k, carry):
            pack(k, g, snd.at[k - 1, g])
            return carry

        lax.fori_loop(k0, k1, body, 0)

    def pack_self(g):
        pack(0, g, rcv.at[0, g])
        first = (a * 4 + x * 2 + c) * MINE
        for i in range(MINE):
            for t in range(3):
                _, two, three = _split(s_ref[t, pl.ds(first + i, GROUP, stride=STRIDE), :])
                hl[0, g, i, :, pl.ds(t * 128, 128)] = two
                hl[1, g, i, :, pl.ds(t * 128, 128)] = three

    m_copy(0).start()
    run_half(0, pl.multiple_of((1 - a) * HALFC, 16), HALFC, False, True)
    pack_range(0, 4, 8)
    h_send(0, 0, FAR)
    h_send(0, 1, FAR)
    m_copy(0).wait_recv()
    m_copy(1).start()
    m_copy(2).start()
    density_rows()
    run_half(0, pl.multiple_of(a * HALFC, 16), HALFC, True, False)
    pack_range(0, 1, 4)
    h_send(0, 0, NEAR)
    h_send(0, 1, NEAR)
    pack_self(0)
    run_half(1, 0, COLS, True, True)
    pack_range(1, 1, 8)
    pack_self(1)
    m_copy(1).wait_recv()
    m_copy(3).start()
    run_half(2, 0, COLS, True, True)
    for k in (4, 6, 2, 5, 7, 3, 1):
        g_copy(k).start()
    for s in (0, 1):
        h_send(1, s)
    pack_range(2, 1, 8)
    for s in (0, 1):
        h_send(2, s)
    pack_self(2)

    met = met_ref[...]
    low, high = _padq(met[:, :QL]), _padq(met[:, QL:])
    own = jnp.where(a == 0, low, high)
    oth = jnp.where(a == 0, high, low)
    m_store(own, 0, 0)
    m_store(oth, 0, QP)
    m_store(jnp.pad(oth, ((0, QP - QL), (0, 0))).T, QP, 0)
    m_copy(2).wait_recv()
    m_copy(3).wait_recv()
    for q in range(3):
        m_store(mr[q], QP + q * MQ, QP)
    m_store(mr[3][4 * MQ - QL:], QP + 3 * MQ, QP)
    for j in range(3):
        m_ref[pl.ds(j * 2 * QP + QL, QP - QL), :] = jnp.zeros((QP - QL, 2 * QP), BF16)
        m_ref[pl.ds(j * 2 * QP + QP + QL, QP - QL), pl.ds(QP, QP)] = jnp.zeros((QP - QL, QP), BF16)

    for k in range(1, 8):
        g_copy(k).wait_recv()
    gam = jnp.concatenate([ga_ref[...] + gr_ref[1] + gr_ref[2] + gr_ref[3],
                           gr_ref[4] + gr_ref[5] + gr_ref[6] + gr_ref[7]], axis=1)

    def stack(v):
        return jnp.concatenate([t.astype(F32) for t in _split(v)], axis=0).astype(BF16)

    def three(v, dot):
        r1, r2, r3 = dot(v, 0), dot(v[:16], 1), dot(v[:8], 2)
        return r1[:8] + ((r1[8:16] + r2[:8]) + (r1[16:] + (r2[8:] + r3)))

    fit = three(stack(gam), lambda v, j: _dot(v, m_ref[pl.ds(j * 2 * QP, 2 * QP), :]))
    weights = three(stack(fit), lambda v, j: _dot(v, m_ref[pl.ds(j * 2 * QP, 2 * QP), pl.ds(0, QP)]))
    wf = jnp.concatenate([t.astype(F32) for t in _split(weights)], axis=0)
    for q in range(4):
        blocks = [jnp.zeros((WPAD * q, QP), F32)] if q else []
        wide = jnp.concatenate(blocks + [wf, jnp.zeros((128 - 24 - WPAD * q, QP), F32)], axis=0)
        wt = wide.T.astype(BF16)
        for j in range(3):
            w_ref[pl.ds((3 * q + j) * QP, QP), :] = wt

    def coulomb(p, carry):
        terms = [t for q in range(4) for t in _split(_padq(b_ref[4 * p + q]))]
        r = _dot(jnp.concatenate(terms, axis=1), w_ref[...]).T
        for q in range(4):
            j_ref[4 * p + q] = r[WPAD * q:WPAD * q + 8] + (r[WPAD * q + 8:WPAD * q + 16] + r[WPAD * q + 16:WPAD * q + 24])
        return carry

    lax.fori_loop(0, ROWS // 4, coulomb, 0)
    for d in range(DENS):
        jd = j_ref[:, d, :]
        jown[d] = jnp.where(a == 0, jd[:, :96], jd[:, 96:])
        jsend[d] = jnp.where(a == 0, jd[:, 96:], jd[:, :96])
    j_copy().start()

    kacc[...] = jnp.zeros_like(kacc)
    xacc[...] = jnp.zeros_like(xacc)

    for s, (i0, n, off, _) in enumerate(SUBSETS):
        if s == 0:
            for g in range(GROUPS):
                h_send(g, 2)
        if s == 1:
            for g in range(GROUPS):
                h_send(g, 3)

        def half(k, g):
            first = rcv[k, g, pl.ds(off, n)].reshape(n * GROUP, 128)
            second = rcv[k, g, pl.ds(off + n, n)].reshape(n * GROUP, 128)
            at, tails = off + 2 * n, []
            for j in range(n // 3):
                p, q = rcv[k, g, at + 2 * j], rcv[k, g, at + 2 * j + 1]
                third = jnp.where(lane < 128 - TAIL, pltpu.roll(p.astype(F32), 128 - TAIL, 1), pltpu.roll(q.astype(F32), 96, 1))
                tails += [p, q, third.astype(BF16)]
            for i in range(n % 3):
                tails.append(rcv[k, g, at + 2 * (n // 3) + i])
            return jnp.concatenate([first, second, jnp.concatenate(tails, axis=0)], axis=1)

        def fit_group(g, carry):
            for k in range(1, 8):
                h_copy(k, g, s).wait_recv()
            lhs = jnp.concatenate([jnp.concatenate([half(k, g), half(k + 4, g)], axis=1) for k in range(4)], axis=0)
            t = _dot(jnp.concatenate([lhs, lhs, lhs], axis=1), m_ref[...])
            h2 = hl[0, g, pl.ds(i0, n)].reshape(n * GROUP, QP)
            h3 = hl[1, g, pl.ds(i0, n)].reshape(n * GROUP, QP)
            ca = _dot(jnp.concatenate([h2, h3], axis=0), m_ref[pl.ds(0, QP), :])
            cb = _dot(h2, m_ref[pl.ds(2 * QP, QP), :])
            w = n * GROUP
            for k in range(4):
                _, px, pc = peer(k)
                part = t[k * w:(k + 1) * w]
                if k == 0:
                    part = part + (ca[:w] + (ca[w:] + cb))
                row = pl.multiple_of((px * 2 + pc) * ROWS + g * GROUP, GROUP)
                t_ref[pl.ds(0, n), pl.ds(row, GROUP), :] = part.reshape(n, GROUP, 2 * QP)
            return carry

        lax.fori_loop(0, GROUPS, fit_group, 0)

        def exchange(i, carry):
            t1, t2, t3 = _split(t_ref[i])
            both = _dot_nt(jnp.concatenate([t1, t2], axis=0), t2)
            kacc[...] += _dot_nt(t1, t1) + both[L:]
            xacc[...] += both[:L] + _dot_nt(t1, t3)
            return carry

        lax.fori_loop(0, n, exchange, 0)

    kacc[...] += xacc[...] + xacc[...].T
    for k in (7, 6, 5, 4, 3, 2, 1, 0):
        pa, px, pc = peer(k)
        rows = kacc[pl.ds(pl.multiple_of((px * 2 + pc) * ROWS, 8), ROWS), :]
        part = jnp.where(pa == 0, rows[:, :96], rows[:, 96:])
        if k:
            ksend[k] = part
        else:
            krecv[0] = part
    for k in (7, 6, 5, 4, 3, 2, 1):
        k_copy(k).start()
    j_copy().wait_recv()
    for k in range(1, 8):
        k_copy(k).wait_recv()
    for k in (0, 2, 4, 6):
        pa, px, _ = peer(k)
        d = pa * 2 + px
        out_ref[d] = 2.0 * (jown[d] + jrecv[d]) - (krecv[k] + krecv[k + 1])

    for k in range(1, 8):
        for g in range(GROUPS):
            for s in range(len(SUBSETS)):
                h_copy(k, g, s).wait_send()
        g_copy(k).wait_send()
        k_copy(k).wait_send()
    for step in range(4):
        m_copy(step).wait_send()
    j_copy().wait_send()


def solution(mesh):
    def local_fock(ints_blk, metric_blk, orbitals):
        bt = jnp.transpose(ints_blk, (1, 2, 0))
        ct = jnp.transpose(orbitals, (0, 2, 1)).reshape(COLS, L)
        ns = len(SUBSETS)
        dma = pltpu.SemaphoreType.DMA
        return pl.pallas_call(
            kernel,
            out_shape=jax.ShapeDtypeStruct((DENS, ROWS, 96), F32),
            in_specs=[pl.BlockSpec(memory_space=pltpu.HBM)] * 3,
            out_specs=pl.BlockSpec(memory_space=pltpu.VMEM),
            scratch_shapes=[
                pltpu.VMEM((ROWS, L, QL), F32),
                pltpu.VMEM((COLS, L), F32),
                pltpu.VMEM((QL, 2 * QL), F32),
                pltpu.VMEM((3, COLS, L), BF16),
                pltpu.VMEM((L, COLS), F32),
                pltpu.VMEM((ROWS, 8, L), F32),
                pltpu.VMEM((3, GROUP * STRIDE, 128), F32),
                pltpu.VMEM((7, GROUPS, SLOTS, GROUP, 128), BF16),
                pltpu.VMEM((8, GROUPS, SLOTS, GROUP, 128), BF16),
                pltpu.VMEM((2, GROUPS, MINE, GROUP, QP), BF16),
                pltpu.VMEM((6 * QP, 2 * QP), BF16),
                pltpu.VMEM((QL, QP), F32),
                pltpu.VMEM((4, MQ, QP), F32),
                pltpu.VMEM((MAXSUB, L, 2 * QP), F32),
                pltpu.VMEM((12 * QP, 128), BF16),
                pltpu.VMEM((8, QP), F32),
                pltpu.VMEM((8, 8, QP), F32),
                pltpu.VMEM((ROWS, 8, L), F32),
                pltpu.VMEM((DENS, ROWS, 96), F32),
                pltpu.VMEM((DENS, ROWS, 96), F32),
                pltpu.VMEM((DENS, ROWS, 96), F32),
                pltpu.VMEM((L, L), F32),
                pltpu.VMEM((L, L), F32),
                pltpu.VMEM((8, ROWS, 96), F32),
                pltpu.VMEM((8, ROWS, 96), F32),
                dma((ROWS // 8,)), dma((2,)), dma((8, GROUPS, ns)), dma((8, GROUPS, ns)), dma((4,)), dma((4,)),
                dma((8,)), dma((8,)), dma, dma, dma((8,)), dma((8,)),
            ],
            compiler_params=pltpu.CompilerParams(collective_id=0, has_side_effects=True, vmem_limit_bytes=50 * 2**20),
            cost_estimate=pl.CostEstimate(flops=25_000_000_000, bytes_accessed=16_000_000, transcendentals=0),
        )(bt, ct, metric_blk)

    return jax.shard_map(local_fock, mesh=mesh, in_specs=(P(('sys', 'aux'), 'orb', None), P(('sys', 'aux'), None), P('sys', None, None)), out_specs=P('sys', 'orb', 'aux'), check_vma=False)
```

```python
import functools

import jax
import jax.numpy as jnp
from jax import lax
from jax.experimental import pallas as pl
from jax.experimental.pallas import tpu as pltpu
from jax.sharding import PartitionSpec as P

MESH = pl.DeviceIdType.MESH
F32, BF16 = jnp.float32, jnp.bfloat16
HIGHEST = lax.Precision.HIGHEST

DENS, L, OCC = 4, 192, 40
COLS = DENS * OCC
MINE = COLS // 8
ROWS = 48
GROUP = 16
GROUPS = ROWS // GROUP
QL, QP = 336, 384
TAIL = QL - 256
STRIDE = 168
HALFC = COLS // 2
MQ = 88
WPAD = 32
NT = (((1,), (1,)), ((), ()))


def _subsets(sizes):
    out, first, off = [], 0, 0
    for n in sizes:
        tails = 2 * (n // 3) + n % 3
        out.append((first, n, off, 2 * n + tails))
        first, off = first + n, off + 2 * n + tails
    return out, off


SUBSETS, SLOTS = _subsets((9, 6, 3, 2))
MAXSUB = max(s[1] for s in SUBSETS)


def _split(v):
    one = v.astype(BF16)
    rest = v - one.astype(F32)
    two = rest.astype(BF16)
    return one, two, (rest - two.astype(F32)).astype(BF16)


def _dot(p, q):
    return jnp.dot(p, q, preferred_element_type=F32)


def _dot_nt(p, q):
    return lax.dot_general(p, q, NT, preferred_element_type=F32)


def _padq(v):
    return jnp.pad(v, ((0, 0), (0, QP - QL)))


def kernel(b_hbm, ct_hbm, met_hbm, out_ref,
           b_ref, ct_ref, met_ref, c_ref, ctt, dm_ref, s_ref, snd, rcv, hl, m_ref, mx, mr, t_ref, w_ref,
           ga_acc, ga_ref, gr_ref, j_ref, jown, jsend, jrecv, kacc, xacc, ksend, krecv,
           bsem, isem, hs_sem, hr_sem, ms_sem, mr_sem, gs_sem, gr_sem, js_sem, jr_sem, ks_sem, kr_sem):
    a = lax.axis_index('aux')
    o = lax.axis_index('orb')
    x, c = o // 2, o % 2
    sys = lax.axis_index('sys')

    def peer(k):
        return (a + k // 4) % 2, (x + (k // 2) % 2) % 2, (c + k % 2) % 2

    def device(k):
        pa, px, pc = peer(k)
        return (sys, pa, px * 2 + pc)

    def remote(src, dst, ssem, rsem, k):
        return pltpu.make_async_remote_copy(src_ref=src, dst_ref=dst, send_sem=ssem, recv_sem=rsem,
                                            device_id=device(k), device_id_type=MESH)

    def b_copy(j):
        return pltpu.make_async_copy(b_hbm.at[pl.ds(j * 8, 8)], b_ref.at[pl.ds(j * 8, 8)], bsem.at[j])

    def h_copy(k, g, s):
        _, _, off, n = SUBSETS[s]
        return remote(snd.at[k - 1, g, pl.ds(off, n)], rcv.at[k, g, pl.ds(off, n)],
                      hs_sem.at[k, g, s], hr_sem.at[k, g, s], k)

    FAR, NEAR = (4, 6, 5, 7), (2, 3, 1)

    def h_send(g, s, ks=(4, 6, 2, 5, 7, 3, 1)):
        for k in ks:
            h_copy(k, g, s).start()

    def m_copy(step):
        mine = o if step < 3 else (1 - x) * 2 + c
        src = mx.at[pl.ds(pl.multiple_of(o * MQ - (o // 3) * (4 * MQ - QL), 8), MQ)] if step == 0 else mr.at[mine]
        return remote(src, mr.at[mine], ms_sem.at[step], mr_sem.at[step], (4, 2, 1, 1)[step])

    def g_copy(k):
        return remote(ga_ref, gr_ref.at[k], gs_sem.at[k], gr_sem.at[k], k)

    def j_copy():
        return remote(jsend, jrecv, js_sem, jr_sem, 4)

    def k_copy(k):
        return remote(ksend.at[k], krecv.at[k], ks_sem.at[k], kr_sem.at[k], k)

    ct_copy = pltpu.make_async_copy(ct_hbm, ct_ref, isem.at[0])
    met_copy = pltpu.make_async_copy(met_hbm, met_ref, isem.at[1])
    ct_copy.start()
    met_copy.start()
    for j in range(ROWS // 8):
        b_copy(j).start()

    barrier = pltpu.get_barrier_semaphore()
    for k in range(1, 8):
        pl.semaphore_signal(barrier, inc=1, device_id=device(k), device_id_type=MESH)

    ct_copy.wait()
    for j, term in enumerate(_split(ct_ref[...])):
        c_ref[j] = term

    met_copy.wait()
    met = met_ref[...]
    low, high = _padq(met[:, :QL]), _padq(met[:, QL:])
    own = jnp.where(a == 0, low, high)
    mx[...] = own
    with jax.named_scope('barrier'):
        pl.semaphore_wait(barrier, 7)

    def m_store(block, row, col):
        for j, term in enumerate(_split(block)):
            m_ref[pl.ds(j * 2 * QP + row, block.shape[0]), pl.ds(col, QP)] = term

    lane = lax.broadcasted_iota(jnp.int32, (GROUP, 128), 1)

    def density_rows():
        ctt[...] = ct_ref[...].T
        rows = ctt[pl.ds(pl.multiple_of(o * ROWS, 8), ROWS), :]
        col = lax.broadcasted_iota(jnp.int32, (ROWS, COLS), 1)
        masked = [jnp.where((col >= d * OCC) & (col < (d + 1) * OCC), rows, 0.0) for d in range(DENS)]
        dens = jnp.dot(jnp.concatenate(masked, axis=0), ct_ref[...], precision=HIGHEST, preferred_element_type=F32)
        dm_ref[...] = jnp.zeros_like(dm_ref)
        for d in range(DENS):
            dm_ref[:, d, :] = dens[d * ROWS:(d + 1) * ROWS]

    def half_transform(g, start, n, with_gamma):
        def body(p, ga):
            m = g * GROUP + 2 * p
            b1, b2, b3 = _split(jnp.concatenate([_padq(b_ref[m]), _padq(b_ref[m + 1])], axis=1))
            terms = [c_ref[j, pl.ds(start, n), :] for j in range(3)]
            if with_gamma:
                extra = _split(dm_ref[pl.ds(m, 2)].reshape(16, L))
                terms = [jnp.concatenate(pair, axis=0) for pair in zip(terms, extra)]
            w = terms[0].shape[0]
            lhs = jnp.concatenate(terms, axis=0)
            r1, r2, r3 = _dot(lhs, b1), _dot(lhs[:2 * w], b2), _dot(lhs[:w], b3)
            h = r1[:w] + ((r1[w:2 * w] + r2[:w]) + (r1[2 * w:] + (r2[w:] + r3)))
            for q in range(2):
                row = pl.multiple_of((2 * p + q) * STRIDE + start, 8)
                for t in range(3):
                    s_ref[t, pl.ds(row, n), :] = h[:n, q * QP + t * 128:q * QP + (t + 1) * 128]
            if with_gamma:
                ga = ga + h[n:n + 8, :QP] + h[n + 8:, QP:]
            return ga

        return body

    def run_half(g, start, n, with_gamma, waits):
        body = half_transform(g, start, n, with_gamma)
        ga = (jnp.zeros((8, QP), F32) if g == 0 else ga_acc[...]) if with_gamma else 0
        for j in range(2):
            if waits:
                b_copy(2 * g + j).wait()
            ga = lax.fori_loop(4 * j, 4 * j + 4, body, ga)
        if with_gamma:
            ga_acc[...] = ga
            if g == GROUPS - 1:
                ga_ref[...] = ga[:DENS]

    def pack(k, g, dst):
        pa, px, pc = peer(k)
        first = (pa * 4 + px * 2 + pc) * MINE

        def load(t, i):
            return s_ref[t, pl.ds(first + i, GROUP, stride=STRIDE), :]

        for i0, n, off, _ in SUBSETS:
            for i in range(n):
                dst[off + i] = load(0, i0 + i).astype(BF16)
                dst[off + n + i] = load(1, i0 + i).astype(BF16)
            at = off + 2 * n
            for j in range(n // 3):
                third = load(2, i0 + 3 * j + 2)
                dst[at + 2 * j] = jnp.where(lane < TAIL, load(2, i0 + 3 * j), pltpu.roll(third, TAIL, 1)).astype(BF16)
                dst[at + 2 * j + 1] = jnp.where(lane < TAIL, load(2, i0 + 3 * j + 1), pltpu.roll(third, 32, 1)).astype(BF16)
            for i in range(n - n % 3, n):
                dst[at + 2 * (n // 3) + i - (n - n % 3)] = load(2, i0 + i).astype(BF16)

    def pack_range(g, k0, k1):
        def body(k, carry):
            pack(k, g, snd.at[k - 1, g])
            return carry

        lax.fori_loop(k0, k1, body, 0)

    def pack_self(g):
        pack(0, g, rcv.at[0, g])
        first = (a * 4 + x * 2 + c) * MINE
        for i in range(MINE):
            for t in range(3):
                _, two, three = _split(s_ref[t, pl.ds(first + i, GROUP, stride=STRIDE), :])
                hl[0, g, i, :, pl.ds(t * 128, 128)] = two
                hl[1, g, i, :, pl.ds(t * 128, 128)] = three

    m_copy(0).start()
    with jax.named_scope('far'):
        run_half(0, pl.multiple_of((1 - a) * HALFC, 16), HALFC, False, True)
    with jax.named_scope('packfar'):
        pack_range(0, 4, 8)
    h_send(0, 0, FAR)
    h_send(0, 1, FAR)
    with jax.named_scope('m0wait'):
        m_copy(0).wait_recv()
    m_copy(1).start()
    m_copy(2).start()
    with jax.named_scope('dens'):
        density_rows()
    with jax.named_scope('near'):
        run_half(0, pl.multiple_of(a * HALFC, 16), HALFC, True, False)
    with jax.named_scope('packnear'):
        pack_range(0, 1, 4)
    h_send(0, 0, NEAR)
    h_send(0, 1, NEAR)
    pack_self(0)
    with jax.named_scope('half1'):
        run_half(1, 0, COLS, True, True)
    with jax.named_scope('pack1'):
        pack_range(1, 1, 8)
    pack_self(1)
    with jax.named_scope('m1wait'):
        m_copy(1).wait_recv()
    m_copy(3).start()
    with jax.named_scope('half2'):
        run_half(2, 0, COLS, True, True)
    for k in (4, 6, 2, 5, 7, 3, 1):
        g_copy(k).start()
    for s in (0, 1):
        h_send(1, s)
    with jax.named_scope('pack2'):
        pack_range(2, 1, 8)
    for s in (0, 1):
        h_send(2, s)
    pack_self(2)

    met = met_ref[...]
    low, high = _padq(met[:, :QL]), _padq(met[:, QL:])
    own = jnp.where(a == 0, low, high)
    oth = jnp.where(a == 0, high, low)
    m_store(own, 0, 0)
    m_store(oth, 0, QP)
    m_store(jnp.pad(oth, ((0, QP - QL), (0, 0))).T, QP, 0)
    with jax.named_scope('m3wait'):
        m_copy(2).wait_recv()
        m_copy(3).wait_recv()
    for q in range(3):
        m_store(mr[q], QP + q * MQ, QP)
    m_store(mr[3][4 * MQ - QL:], QP + 3 * MQ, QP)
    for j in range(3):
        m_ref[pl.ds(j * 2 * QP + QL, QP - QL), :] = jnp.zeros((QP - QL, 2 * QP), BF16)
        m_ref[pl.ds(j * 2 * QP + QP + QL, QP - QL), pl.ds(QP, QP)] = jnp.zeros((QP - QL, QP), BF16)

    with jax.named_scope('gwait'):
        for k in range(1, 8):
            g_copy(k).wait_recv()
    gam = jnp.concatenate([ga_ref[...] + gr_ref[1] + gr_ref[2] + gr_ref[3],
                           gr_ref[4] + gr_ref[5] + gr_ref[6] + gr_ref[7]], axis=1)
    gam = jnp.concatenate([gam, jnp.zeros_like(gam)], axis=0)

    def stack(v):
        return jnp.concatenate([t.astype(F32) for t in _split(v)], axis=0).astype(BF16)

    def three(v, dot):
        r1, r2, r3 = dot(v, 0), dot(v[:16], 1), dot(v[:8], 2)
        return r1[:8] + ((r1[8:16] + r2[:8]) + (r1[16:] + (r2[8:] + r3)))

    fit = three(stack(gam), lambda v, j: _dot(v, m_ref[pl.ds(j * 2 * QP, 2 * QP), :]))
    weights = three(stack(fit), lambda v, j: _dot(v, m_ref[pl.ds(j * 2 * QP, 2 * QP), pl.ds(0, QP)]))
    wf = jnp.concatenate([t.astype(F32) for t in _split(weights)], axis=0)
    for q in range(4):
        blocks = [jnp.zeros((WPAD * q, QP), F32)] if q else []
        wide = jnp.concatenate(blocks + [wf, jnp.zeros((128 - 24 - WPAD * q, QP), F32)], axis=0)
        wt = wide.T.astype(BF16)
        for j in range(3):
            w_ref[pl.ds((3 * q + j) * QP, QP), :] = wt

    def coulomb(p, carry):
        terms = [t for q in range(4) for t in _split(_padq(b_ref[4 * p + q]))]
        r = _dot(jnp.concatenate(terms, axis=1), w_ref[...]).T
        for q in range(4):
            j_ref[4 * p + q] = r[WPAD * q:WPAD * q + 8] + (r[WPAD * q + 8:WPAD * q + 16] + r[WPAD * q + 16:WPAD * q + 24])
        return carry

    with jax.named_scope('coulomb'):
        lax.fori_loop(0, ROWS // 4, coulomb, 0)
    away = []
    for d in range(DENS):
        jd = j_ref[:, d, :]
        jown[d] = jnp.where(a == 0, jd[:, :96], jd[:, 96:])
        away.append(jnp.where(a == 0, jd[:, 96:], jd[:, :96]))
    jsend[...] = jnp.concatenate(away, axis=1)
    j_copy().start()

    kacc[...] = jnp.zeros_like(kacc)
    xacc[...] = jnp.zeros_like(xacc)

    for s, (i0, n, off, _) in enumerate(SUBSETS):
        if s == 0:
            for g in range(GROUPS):
                h_send(g, 2)
        if s == 1:
            for g in range(GROUPS):
                h_send(g, 3)

        def half(k, g):
            first = rcv[k, g, pl.ds(off, n)].reshape(n * GROUP, 128)
            second = rcv[k, g, pl.ds(off + n, n)].reshape(n * GROUP, 128)
            at, tails = off + 2 * n, []
            for j in range(n // 3):
                p, q = rcv[k, g, at + 2 * j], rcv[k, g, at + 2 * j + 1]
                third = jnp.where(lane < 128 - TAIL, pltpu.roll(p.astype(F32), 128 - TAIL, 1), pltpu.roll(q.astype(F32), 96, 1))
                tails += [p, q, third.astype(BF16)]
            for i in range(n % 3):
                tails.append(rcv[k, g, at + 2 * (n // 3) + i])
            return jnp.concatenate([first, second, jnp.concatenate(tails, axis=0)], axis=1)

        def fit_group(g, carry):
            with jax.named_scope(f'hwait{s}'):
                for k in range(1, 8):
                    h_copy(k, g, s).wait_recv()
            lhs = jnp.concatenate([jnp.concatenate([half(k, g), half(k + 4, g)], axis=1) for k in range(4)], axis=0)
            t = _dot(jnp.concatenate([lhs, lhs, lhs], axis=1), m_ref[...])
            h2 = hl[0, g, pl.ds(i0, n)].reshape(n * GROUP, QP)
            h3 = hl[1, g, pl.ds(i0, n)].reshape(n * GROUP, QP)
            ca = _dot(jnp.concatenate([h2, h3], axis=0), m_ref[pl.ds(0, QP), :])
            cb = _dot(h2, m_ref[pl.ds(2 * QP, QP), :])
            w = n * GROUP
            for k in range(4):
                _, px, pc = peer(k)
                part = t[k * w:(k + 1) * w]
                if k == 0:
                    part = part + (ca[:w] + (ca[w:] + cb))
                row = pl.multiple_of((px * 2 + pc) * ROWS + g * GROUP, GROUP)
                t_ref[pl.ds(0, n), pl.ds(row, GROUP), :] = part.reshape(n, GROUP, 2 * QP)
            return carry

        with jax.named_scope(f'fit{s}'):
            lax.fori_loop(0, GROUPS, fit_group, 0)

        def exchange(i, carry):
            t1, t2, t3 = _split(t_ref[i])
            both = _dot_nt(jnp.concatenate([t1, t2], axis=0), t2)
            kacc[...] += _dot_nt(t1, t1) + both[L:]
            xacc[...] += both[:L] + _dot_nt(t1, t3)
            return carry

        with jax.named_scope(f'exch{s}'):
            lax.fori_loop(0, n, exchange, 0)

    j_copy().wait_recv()
    theirs = jrecv[...]
    for d in range(DENS):
        jown[d] = 2.0 * (jown[d] + theirs[:, 96 * d:96 * (d + 1)])
    kacc[...] += xacc[...] + xacc[...].T
    for k in (7, 6, 5, 4, 3, 2, 1, 0):
        pa, px, pc = peer(k)
        rows = kacc[pl.ds(pl.multiple_of((px * 2 + pc) * ROWS, 8), ROWS), :]
        part = jnp.where(pa == 0, rows[:, :96], rows[:, 96:])
        if k:
            ksend[k] = part
        else:
            krecv[0] = part
    for k in (7, 6, 5, 4, 3, 2, 1):
        k_copy(k).start()
    with jax.named_scope('kwait'):
        for k in range(1, 8):
            k_copy(k).wait_recv()
    for k in (0, 2, 4, 6):
        pa, px, _ = peer(k)
        d = pa * 2 + px
        out_ref[d] = jown[d] - (krecv[k] + krecv[k + 1])

    for k in range(1, 8):
        for g in range(GROUPS):
            for s in range(len(SUBSETS)):
                h_copy(k, g, s).wait_send()
        g_copy(k).wait_send()
        k_copy(k).wait_send()
    for step in range(4):
        m_copy(step).wait_send()
    j_copy().wait_send()


def solution(mesh):
    def local_fock(ints_blk, metric_blk, orbitals):
        bt = jnp.transpose(ints_blk, (1, 2, 0))
        ct = jnp.transpose(orbitals, (0, 2, 1)).reshape(COLS, L)
        ns = len(SUBSETS)
        dma = pltpu.SemaphoreType.DMA
        return pl.pallas_call(
            kernel,
            out_shape=jax.ShapeDtypeStruct((DENS, ROWS, 96), F32),
            in_specs=[pl.BlockSpec(memory_space=pltpu.HBM)] * 3,
            out_specs=pl.BlockSpec(memory_space=pltpu.VMEM),
            scratch_shapes=[
                pltpu.VMEM((ROWS, L, QL), F32),
                pltpu.VMEM((COLS, L), F32),
                pltpu.VMEM((QL, 2 * QL), F32),
                pltpu.VMEM((3, COLS, L), BF16),
                pltpu.VMEM((L, COLS), F32),
                pltpu.VMEM((ROWS, 8, L), F32),
                pltpu.VMEM((3, GROUP * STRIDE, 128), F32),
                pltpu.VMEM((7, GROUPS, SLOTS, GROUP, 128), BF16),
                pltpu.VMEM((8, GROUPS, SLOTS, GROUP, 128), BF16),
                pltpu.VMEM((2, GROUPS, MINE, GROUP, QP), BF16),
                pltpu.VMEM((6 * QP, 2 * QP), BF16),
                pltpu.VMEM((QL, QP), F32),
                pltpu.VMEM((4, MQ, QP), F32),
                pltpu.VMEM((MAXSUB, L, 2 * QP), F32),
                pltpu.VMEM((12 * QP, 128), BF16),
                pltpu.VMEM((8, QP), F32),
                pltpu.VMEM((DENS, QP), F32),
                pltpu.VMEM((8, DENS, QP), F32),
                pltpu.VMEM((ROWS, 8, L), F32),
                pltpu.VMEM((DENS, ROWS, 96), F32),
                pltpu.VMEM((ROWS, DENS * 96), F32),
                pltpu.VMEM((ROWS, DENS * 96), F32),
                pltpu.VMEM((L, L), F32),
                pltpu.VMEM((L, L), F32),
                pltpu.VMEM((8, ROWS, 96), F32),
                pltpu.VMEM((8, ROWS, 96), F32),
                dma((ROWS // 8,)), dma((2,)), dma((8, GROUPS, ns)), dma((8, GROUPS, ns)), dma((4,)), dma((4,)),
                dma((8,)), dma((8,)), dma, dma, dma((8,)), dma((8,)),
            ],
            compiler_params=pltpu.CompilerParams(collective_id=0, has_side_effects=True, vmem_limit_bytes=56_360_000),
            cost_estimate=pl.CostEstimate(flops=25_000_000_000, bytes_accessed=16_000_000, transcendentals=0),
        )(bt, ct, metric_blk)

    return jax.shard_map(local_fock, mesh=mesh, in_specs=(P(('sys', 'aux'), 'orb', None), P(('sys', 'aux'), None), P('sys', None, None)), out_specs=P('sys', 'orb', 'aux'), check_vma=False)
```

```python
import functools

import jax
import jax.numpy as jnp
from jax import lax
from jax.experimental import pallas as pl
from jax.experimental.pallas import tpu as pltpu
from jax.sharding import PartitionSpec as P

MESH = pl.DeviceIdType.MESH
F32, BF16 = jnp.float32, jnp.bfloat16
HIGHEST = lax.Precision.HIGHEST

DENS, L, OCC = 4, 192, 40
COLS = DENS * OCC
MINE = COLS // 8
ROWS = 48
GROUP = 16
GROUPS = ROWS // GROUP
QL, QP = 336, 384
TAIL = QL - 256
STRIDE = 168
HALFC = COLS // 2
MQ = 88
WPAD = 32
NT = (((1,), (1,)), ((), ()))


def _subsets(sizes):
    out, first, off = [], 0, 0
    for n in sizes:
        tails = 2 * (n // 3) + n % 3
        out.append((first, n, off, 2 * n + tails))
        first, off = first + n, off + 2 * n + tails
    return out, off


SUBSETS, SLOTS = _subsets((9, 6, 3, 2))
MAXSUB = max(s[1] for s in SUBSETS)


def _split(v):
    one = v.astype(BF16)
    rest = v - one.astype(F32)
    two = rest.astype(BF16)
    return one, two, (rest - two.astype(F32)).astype(BF16)


def _dot(p, q):
    return jnp.dot(p, q, preferred_element_type=F32)


def _dot_nt(p, q):
    return lax.dot_general(p, q, NT, preferred_element_type=F32)


def _padq(v):
    return jnp.pad(v, ((0, 0), (0, QP - QL)))


def kernel(b_hbm, ct_hbm, met_hbm, out_ref,
           b_ref, ct_ref, met_ref, c_ref, ctt, dm_ref, s_ref, snd, rcv, hl, m_ref, mx, mr, t_ref, w_ref,
           ga_acc, ga_ref, gr_ref, j_ref, jown, jsend, jrecv, kacc, xacc, ksend, krecv,
           bsem, isem, hs_sem, hr_sem, ms_sem, mr_sem, gs_sem, gr_sem, js_sem, jr_sem, ks_sem, kr_sem):
    a = lax.axis_index('aux')
    o = lax.axis_index('orb')
    x, c = o // 2, o % 2
    sys = lax.axis_index('sys')

    def peer(k):
        return (a + k // 4) % 2, (x + (k // 2) % 2) % 2, (c + k % 2) % 2

    def device(k):
        pa, px, pc = peer(k)
        return (sys, pa, px * 2 + pc)

    def remote(src, dst, ssem, rsem, k):
        return pltpu.make_async_remote_copy(src_ref=src, dst_ref=dst, send_sem=ssem, recv_sem=rsem,
                                            device_id=device(k), device_id_type=MESH)

    def b_copy(j):
        return pltpu.make_async_copy(b_hbm.at[pl.ds(j * 8, 8)], b_ref.at[pl.ds(j * 8, 8)], bsem.at[j])

    def h_copy(k, g, s):
        _, _, off, n = SUBSETS[s]
        return remote(snd.at[k - 1, g, pl.ds(off, n)], rcv.at[k, g, pl.ds(off, n)],
                      hs_sem.at[k, g, s], hr_sem.at[k, g, s], k)

    FAR, NEAR = (4, 6, 5, 7), (2, 3, 1)

    def h_send(g, s, ks=(4, 6, 2, 5, 7, 3, 1)):
        for k in ks:
            h_copy(k, g, s).start()

    def m_copy(step):
        mine = o if step < 3 else (1 - x) * 2 + c
        src = mx.at[pl.ds(pl.multiple_of(o * MQ - (o // 3) * (4 * MQ - QL), 8), MQ)] if step == 0 else mr.at[mine]
        return remote(src, mr.at[mine], ms_sem.at[step], mr_sem.at[step], (4, 2, 1, 1)[step])

    def g_copy(k):
        return remote(ga_ref, gr_ref.at[k], gs_sem.at[k], gr_sem.at[k], k)

    def j_copy():
        return remote(jsend, jrecv, js_sem, jr_sem, 4)

    def k_copy(k):
        return remote(ksend.at[k], krecv.at[k], ks_sem.at[k], kr_sem.at[k], k)

    ct_copy = pltpu.make_async_copy(ct_hbm, ct_ref, isem.at[0])
    met_copy = pltpu.make_async_copy(met_hbm, met_ref, isem.at[1])
    ct_copy.start()
    met_copy.start()
    for j in range(2):
        b_copy(j).start()

    barrier = pltpu.get_barrier_semaphore()
    for k in range(1, 8):
        pl.semaphore_signal(barrier, inc=1, device_id=device(k), device_id_type=MESH)

    ct_copy.wait()
    for j, term in enumerate(_split(ct_ref[...])):
        c_ref[j] = term

    met_copy.wait()
    met = met_ref[...]
    low, high = _padq(met[:, :QL]), _padq(met[:, QL:])
    own = jnp.where(a == 0, low, high)
    mx[...] = own
    with jax.named_scope('barrier'):
        pl.semaphore_wait(barrier, 7)

    def m_store(block, row, col):
        for j, term in enumerate(_split(block)):
            m_ref[pl.ds(j * 2 * QP + row, block.shape[0]), pl.ds(col, QP)] = term

    lane = lax.broadcasted_iota(jnp.int32, (GROUP, 128), 1)

    def density_rows():
        ctt[...] = ct_ref[...].T
        rows = ctt[pl.ds(pl.multiple_of(o * ROWS, 8), ROWS), :]
        col = lax.broadcasted_iota(jnp.int32, (ROWS, COLS), 1)
        masked = [jnp.where((col >= d * OCC) & (col < (d + 1) * OCC), rows, 0.0) for d in range(DENS)]
        dens = jnp.dot(jnp.concatenate(masked, axis=0), ct_ref[...], precision=HIGHEST, preferred_element_type=F32)
        dm_ref[...] = jnp.zeros_like(dm_ref)
        for d in range(DENS):
            dm_ref[:, d, :] = dens[d * ROWS:(d + 1) * ROWS]

    def half_transform(g, start, n, with_gamma):
        def body(p, ga):
            m = g * GROUP + 2 * p
            b1, b2, b3 = _split(jnp.concatenate([_padq(b_ref[m]), _padq(b_ref[m + 1])], axis=1))
            terms = [c_ref[j, pl.ds(start, n), :] for j in range(3)]
            if with_gamma:
                extra = _split(dm_ref[pl.ds(m, 2)].reshape(16, L))
                terms = [jnp.concatenate(pair, axis=0) for pair in zip(terms, extra)]
            w = terms[0].shape[0]
            lhs = jnp.concatenate(terms, axis=0)
            r1, r2, r3 = _dot(lhs, b1), _dot(lhs[:2 * w], b2), _dot(lhs[:w], b3)
            h = r1[:w] + ((r1[w:2 * w] + r2[:w]) + (r1[2 * w:] + (r2[w:] + r3)))
            for q in range(2):
                row = pl.multiple_of((2 * p + q) * STRIDE + start, 8)
                for t in range(3):
                    s_ref[t, pl.ds(row, n), :] = h[:n, q * QP + t * 128:q * QP + (t + 1) * 128]
            if with_gamma:
                ga = ga + h[n:n + 8, :QP] + h[n + 8:, QP:]
            return ga

        return body

    def run_half(g, start, n, with_gamma, waits):
        body = half_transform(g, start, n, with_gamma)
        ga = (jnp.zeros((8, QP), F32) if g == 0 else ga_acc[...]) if with_gamma else 0
        for j in range(2):
            if waits:
                b_copy(2 * g + j).wait()
                if 2 * g + j == 1:
                    for later in range(2, ROWS // 8):
                        b_copy(later).start()
            ga = lax.fori_loop(2 * j, 2 * j + 2, lambda p, v: body(2 * p + 1, body(2 * p, v)), ga)
        if with_gamma:
            ga_acc[...] = ga
            if g == GROUPS - 1:
                ga_ref[...] = ga[:DENS]

    def pack(k, g, dst):
        pa, px, pc = peer(k)
        first = (pa * 4 + px * 2 + pc) * MINE

        def load(t, i):
            return s_ref[t, pl.ds(first + i, GROUP, stride=STRIDE), :]

        for i0, n, off, _ in SUBSETS:
            for i in range(n):
                dst[off + i] = load(0, i0 + i).astype(BF16)
                dst[off + n + i] = load(1, i0 + i).astype(BF16)
            at = off + 2 * n
            for j in range(n // 3):
                third = load(2, i0 + 3 * j + 2)
                dst[at + 2 * j] = jnp.where(lane < TAIL, load(2, i0 + 3 * j), pltpu.roll(third, TAIL, 1)).astype(BF16)
                dst[at + 2 * j + 1] = jnp.where(lane < TAIL, load(2, i0 + 3 * j + 1), pltpu.roll(third, 32, 1)).astype(BF16)
            for i in range(n - n % 3, n):
                dst[at + 2 * (n // 3) + i - (n - n % 3)] = load(2, i0 + i).astype(BF16)

    def pack_range(g, k0, k1):
        def body(k, carry):
            pack(k, g, snd.at[k - 1, g])
            return carry

        lax.fori_loop(k0, k1, body, 0)

    def pack_self(g):
        pack(0, g, rcv.at[0, g])
        first = (a * 4 + x * 2 + c) * MINE
        for i in range(MINE):
            for t in range(3):
                _, two, three = _split(s_ref[t, pl.ds(first + i, GROUP, stride=STRIDE), :])
                hl[0, g, i, :, pl.ds(t * 128, 128)] = two
                hl[1, g, i, :, pl.ds(t * 128, 128)] = three

    scope = jax.named_scope
    m_copy(0).start()
    with scope('far'):
        run_half(0, pl.multiple_of((1 - a) * HALFC, 16), HALFC, False, True)
    with scope('packfar'):
        pack_range(0, 4, 8)
    h_send(0, 0, FAR)
    h_send(0, 1, FAR)
    with scope('dens'):
        density_rows()
    with scope('near'):
        run_half(0, pl.multiple_of(a * HALFC, 16), HALFC, True, False)
    with scope('packnear'):
        pack_range(0, 1, 4)
    with scope('m0wait'):
        m_copy(0).wait_recv()
    m_copy(1).start()
    m_copy(2).start()
    h_send(0, 0, NEAR)
    h_send(0, 1, NEAR)
    pack_self(0)
    with scope('half1'):
        run_half(1, 0, COLS, True, True)
    with scope('pack1'):
        pack_range(1, 1, 8)
    pack_self(1)
    with scope('half2'):
        run_half(2, 0, COLS, True, True)
    for k in (4, 6, 2, 5, 7, 3, 1):
        g_copy(k).start()
    for s in (0, 1):
        h_send(1, s)
    with scope('pack2'):
        pack_range(2, 1, 8)
    for s in (0, 1):
        h_send(2, s)
    with scope('m1wait'):
        m_copy(1).wait_recv()
    m_copy(3).start()
    pack_self(2)

    met = met_ref[...]
    low, high = _padq(met[:, :QL]), _padq(met[:, QL:])
    own = jnp.where(a == 0, low, high)
    oth = jnp.where(a == 0, high, low)
    m_store(own, 0, 0)
    m_store(oth, 0, QP)
    m_store(jnp.pad(oth, ((0, QP - QL), (0, 0))).T, QP, 0)
    with jax.named_scope('m3wait'):
        m_copy(2).wait_recv()
        m_copy(3).wait_recv()
    for q in range(3):
        m_store(mr[q], QP + q * MQ, QP)
    m_store(mr[3][4 * MQ - QL:], QP + 3 * MQ, QP)
    for j in range(3):
        m_ref[pl.ds(j * 2 * QP + QL, QP - QL), :] = jnp.zeros((QP - QL, 2 * QP), BF16)
        m_ref[pl.ds(j * 2 * QP + QP + QL, QP - QL), pl.ds(QP, QP)] = jnp.zeros((QP - QL, QP), BF16)

    with jax.named_scope('gwait'):
        for k in range(1, 8):
            g_copy(k).wait_recv()
    for g in range(GROUPS):
        h_send(g, 2)
    gam = jnp.concatenate([ga_ref[...] + gr_ref[1] + gr_ref[2] + gr_ref[3],
                           gr_ref[4] + gr_ref[5] + gr_ref[6] + gr_ref[7]], axis=1)
    gam = jnp.concatenate([gam, jnp.zeros_like(gam)], axis=0)

    def stack(v):
        return jnp.concatenate([t.astype(F32) for t in _split(v)], axis=0).astype(BF16)

    def three(v, dot):
        r1, r2, r3 = dot(v, 0), dot(v[:16], 1), dot(v[:8], 2)
        return r1[:8] + ((r1[8:16] + r2[:8]) + (r1[16:] + (r2[8:] + r3)))

    fit = three(stack(gam), lambda v, j: _dot(v, m_ref[pl.ds(j * 2 * QP, 2 * QP), :]))
    weights = three(stack(fit), lambda v, j: _dot(v, m_ref[pl.ds(j * 2 * QP, 2 * QP), pl.ds(0, QP)]))
    wf = jnp.concatenate([t.astype(F32) for t in _split(weights)], axis=0)
    for q in range(4):
        blocks = [jnp.zeros((WPAD * q, QP), F32)] if q else []
        wide = jnp.concatenate(blocks + [wf, jnp.zeros((128 - 24 - WPAD * q, QP), F32)], axis=0)
        wt = wide.T.astype(BF16)
        for j in range(3):
            w_ref[pl.ds((3 * q + j) * QP, QP), :] = wt

    def coulomb(p, carry):
        terms = [t for q in range(4) for t in _split(_padq(b_ref[4 * p + q]))]
        r = _dot(jnp.concatenate(terms, axis=1), w_ref[...]).T
        for q in range(4):
            j_ref[4 * p + q] = r[WPAD * q:WPAD * q + 8] + (r[WPAD * q + 8:WPAD * q + 16] + r[WPAD * q + 16:WPAD * q + 24])
        return carry

    with jax.named_scope('coulomb'):
        lax.fori_loop(0, ROWS // 4, coulomb, 0)
    away = []
    for d in range(DENS):
        jd = j_ref[:, d, :]
        jown[d] = jnp.where(a == 0, jd[:, :96], jd[:, 96:])
        away.append(jnp.where(a == 0, jd[:, 96:], jd[:, :96]))
    jsend[...] = jnp.concatenate(away, axis=1)
    j_copy().start()
    for g in range(GROUPS):
        h_send(g, 3)

    kacc[...] = jnp.zeros_like(kacc)
    xacc[...] = jnp.zeros_like(xacc)

    for s, (i0, n, off, _) in enumerate(SUBSETS):

        def half(k, g):
            first = rcv[k, g, pl.ds(off, n)].reshape(n * GROUP, 128)
            second = rcv[k, g, pl.ds(off + n, n)].reshape(n * GROUP, 128)
            at, tails = off + 2 * n, []
            for j in range(n // 3):
                p, q = rcv[k, g, at + 2 * j], rcv[k, g, at + 2 * j + 1]
                third = jnp.where(lane < 128 - TAIL, pltpu.roll(p.astype(F32), 128 - TAIL, 1), pltpu.roll(q.astype(F32), 96, 1))
                tails += [p, q, third.astype(BF16)]
            for i in range(n % 3):
                tails.append(rcv[k, g, at + 2 * (n // 3) + i])
            return jnp.concatenate([first, second, jnp.concatenate(tails, axis=0)], axis=1)

        def fit_group(g, carry):
            with jax.named_scope(f'hwait{s}'):
                for k in range(1, 8):
                    h_copy(k, g, s).wait_recv()
            lhs = jnp.concatenate([jnp.concatenate([half(k, g), half(k + 4, g)], axis=1) for k in range(4)], axis=0)
            t = _dot(jnp.concatenate([lhs, lhs, lhs], axis=1), m_ref[...])
            h2 = hl[0, g, pl.ds(i0, n)].reshape(n * GROUP, QP)
            h3 = hl[1, g, pl.ds(i0, n)].reshape(n * GROUP, QP)
            ca = _dot(jnp.concatenate([h2, h3], axis=0), m_ref[pl.ds(0, QP), :])
            cb = _dot(h2, m_ref[pl.ds(2 * QP, QP), :])
            w = n * GROUP
            for k in range(4):
                _, px, pc = peer(k)
                part = t[k * w:(k + 1) * w]
                if k == 0:
                    part = part + (ca[:w] + (ca[w:] + cb))
                row = pl.multiple_of((px * 2 + pc) * ROWS + g * GROUP, GROUP)
                t_ref[pl.ds(0, n), pl.ds(row, GROUP), :] = part.reshape(n, GROUP, 2 * QP)
            return carry

        with jax.named_scope(f'fit{s}'):
            lax.fori_loop(0, GROUPS, fit_group, 0)

        step = 3 if n % 3 == 0 else 2

        def exchange(i, carry):
            terms = zip(*[_split(t_ref[step * i + j]) for j in range(step)])
            t1, t2, t3 = [jnp.concatenate(v, axis=1) for v in terms]
            both = _dot_nt(jnp.concatenate([t1, t2], axis=0), t2)
            kacc[...] += _dot_nt(t1, t1) + both[L:]
            xacc[...] += both[:L] + _dot_nt(t1, t3)
            return carry

        with jax.named_scope(f'exch{s}'):
            lax.fori_loop(0, n // step, exchange, 0)

    j_copy().wait_recv()
    theirs = jrecv[...]
    for d in range(DENS):
        jown[d] = 2.0 * (jown[d] + theirs[:, 96 * d:96 * (d + 1)])
    kacc[...] += xacc[...] + xacc[...].T
    for k in (7, 6, 5, 4, 3, 2, 1, 0):
        pa, px, pc = peer(k)
        rows = kacc[pl.ds(pl.multiple_of((px * 2 + pc) * ROWS, 8), ROWS), :]
        part = jnp.where(pa == 0, rows[:, :96], rows[:, 96:])
        if k:
            ksend[k] = part
        else:
            krecv[0] = part
    for k in (7, 6, 5, 4, 3, 2, 1):
        k_copy(k).start()
    with jax.named_scope('kwait'):
        for k in range(1, 8):
            k_copy(k).wait_recv()
    for k in (0, 2, 4, 6):
        pa, px, _ = peer(k)
        d = pa * 2 + px
        out_ref[d] = jown[d] - (krecv[k] + krecv[k + 1])

    for k in range(1, 8):
        for g in range(GROUPS):
            for s in range(len(SUBSETS)):
                h_copy(k, g, s).wait_send()
        g_copy(k).wait_send()
        k_copy(k).wait_send()
    for step in range(4):
        m_copy(step).wait_send()
    j_copy().wait_send()


def solution(mesh):
    def local_fock(ints_blk, metric_blk, orbitals):
        bt = jnp.transpose(ints_blk, (1, 2, 0))
        ct = jnp.transpose(orbitals, (0, 2, 1)).reshape(COLS, L)
        ns = len(SUBSETS)
        dma = pltpu.SemaphoreType.DMA
        return pl.pallas_call(
            kernel,
            out_shape=jax.ShapeDtypeStruct((DENS, ROWS, 96), F32),
            in_specs=[pl.BlockSpec(memory_space=pltpu.HBM)] * 3,
            out_specs=pl.BlockSpec(memory_space=pltpu.VMEM),
            scratch_shapes=[
                pltpu.VMEM((ROWS, L, QL), F32),
                pltpu.VMEM((COLS, L), F32),
                pltpu.VMEM((QL, 2 * QL), F32),
                pltpu.VMEM((3, COLS, L), BF16),
                pltpu.VMEM((L, COLS), F32),
                pltpu.VMEM((ROWS, 8, L), F32),
                pltpu.VMEM((3, GROUP * STRIDE, 128), F32),
                pltpu.VMEM((7, GROUPS, SLOTS, GROUP, 128), BF16),
                pltpu.VMEM((8, GROUPS, SLOTS, GROUP, 128), BF16),
                pltpu.VMEM((2, GROUPS, MINE, GROUP, QP), BF16),
                pltpu.VMEM((6 * QP, 2 * QP), BF16),
                pltpu.VMEM((QL, QP), F32),
                pltpu.VMEM((4, MQ, QP), F32),
                pltpu.VMEM((MAXSUB, L, 2 * QP), F32),
                pltpu.VMEM((12 * QP, 128), BF16),
                pltpu.VMEM((8, QP), F32),
                pltpu.VMEM((DENS, QP), F32),
                pltpu.VMEM((8, DENS, QP), F32),
                pltpu.VMEM((ROWS, 8, L), F32),
                pltpu.VMEM((DENS, ROWS, 96), F32),
                pltpu.VMEM((ROWS, DENS * 96), F32),
                pltpu.VMEM((ROWS, DENS * 96), F32),
                pltpu.VMEM((L, L), F32),
                pltpu.VMEM((L, L), F32),
                pltpu.VMEM((8, ROWS, 96), F32),
                pltpu.VMEM((8, ROWS, 96), F32),
                dma((ROWS // 8,)), dma((2,)), dma((8, GROUPS, ns)), dma((8, GROUPS, ns)), dma((4,)), dma((4,)),
                dma((8,)), dma((8,)), dma, dma, dma((8,)), dma((8,)),
            ],
            compiler_params=pltpu.CompilerParams(collective_id=0, has_side_effects=True, vmem_limit_bytes=56_360_000),
            cost_estimate=pl.CostEstimate(flops=25_000_000_000, bytes_accessed=16_000_000, transcendentals=0),
        )(bt, ct, metric_blk)

    return jax.shard_map(local_fock, mesh=mesh, in_specs=(P(('sys', 'aux'), 'orb', None), P(('sys', 'aux'), None), P('sys', None, None)), out_specs=P('sys', 'orb', 'aux'), check_vma=False)
```

```python
import functools

import jax
import jax.numpy as jnp
from jax import lax
from jax.experimental import pallas as pl
from jax.experimental.pallas import tpu as pltpu
from jax.sharding import PartitionSpec as P

MESH = pl.DeviceIdType.MESH
F32, BF16 = jnp.float32, jnp.bfloat16
HIGHEST = lax.Precision.HIGHEST

DENS, L, OCC = 4, 192, 40
COLS = DENS * OCC
MINE = COLS // 8
ROWS = 48
GROUP = 16
GROUPS = ROWS // GROUP
QL, QP = 336, 384
TAIL = QL - 256
STRIDE = 168
HALFC = COLS // 2
MQ = 88
WPAD = 32
NT = (((1,), (1,)), ((), ()))


def _subsets(sizes):
    out, first, off = [], 0, 0
    for n in sizes:
        tails = 2 * (n // 3) + n % 3
        out.append((first, n, off, 2 * n + tails))
        first, off = first + n, off + 2 * n + tails
    return out, off


SUBSETS, SLOTS = _subsets((9, 6, 3, 2))
MAXSUB = max(s[1] for s in SUBSETS)


def _split(v):
    one = v.astype(BF16)
    rest = v - one.astype(F32)
    two = rest.astype(BF16)
    return one, two, (rest - two.astype(F32)).astype(BF16)


def _dot(p, q):
    return jnp.dot(p, q, preferred_element_type=F32)


def _dot_nt(p, q):
    return lax.dot_general(p, q, NT, preferred_element_type=F32)


def _padq(v):
    return jnp.pad(v, ((0, 0), (0, QP - QL)))


def kernel(b_hbm, ct_hbm, met_hbm, out_ref,
           b_ref, ct_ref, met_ref, c_ref, ctt, dm_ref, s_ref, snd, rcv, hl, m_ref, mx, mr, t_ref, w_ref,
           ga_acc, ga_ref, gr_ref, j_ref, jown, jsend, jrecv, kacc, xacc, ksend, krecv,
           bsem, isem, hs_sem, hr_sem, ms_sem, mr_sem, gs_sem, gr_sem, js_sem, jr_sem, ks_sem, kr_sem):
    a = lax.axis_index('aux')
    o = lax.axis_index('orb')
    x, c = o // 2, o % 2
    sys = lax.axis_index('sys')

    def peer(k):
        return (a + k // 4) % 2, (x + (k // 2) % 2) % 2, (c + k % 2) % 2

    def device(k):
        pa, px, pc = peer(k)
        return (sys, pa, px * 2 + pc)

    def remote(src, dst, ssem, rsem, k):
        return pltpu.make_async_remote_copy(src_ref=src, dst_ref=dst, send_sem=ssem, recv_sem=rsem,
                                            device_id=device(k), device_id_type=MESH)

    def b_copy(j):
        first, n = ((0, 8), (8, 8), (16, 16), (32, 16))[j]
        return pltpu.make_async_copy(b_hbm.at[pl.ds(first, n)], b_ref.at[pl.ds(first, n)], bsem.at[j])

    def all_sent(ref, sem):
        remote(ref, ref, sem, sem, 0).wait_send()

    def all_here(ref, sem):
        remote(ref, ref, sem, sem, 0).wait_recv()

    def h_copy(k, g, s):
        _, _, off, n = SUBSETS[s]
        return remote(snd.at[k - 1, g, pl.ds(off, n)], rcv.at[k, g, pl.ds(off, n)],
                      hs_sem, hr_sem.at[g, s], k)

    FAR, NEAR = (4, 6, 5, 7), (2, 3, 1)

    def h_send(g, s, ks=(4, 6, 2, 5, 7, 3, 1)):
        for k in ks:
            h_copy(k, g, s).start()

    def m_copy(step):
        mine = o if step < 3 else (1 - x) * 2 + c
        src = mx.at[pl.ds(pl.multiple_of(o * MQ - (o // 3) * (4 * MQ - QL), 8), MQ)] if step == 0 else mr.at[mine]
        return remote(src, mr.at[mine], ms_sem, mr_sem.at[min(step, 2)], (4, 2, 1, 1)[step])

    def g_copy(k):
        return remote(ga_ref, gr_ref.at[k], gs_sem, gr_sem, k)

    def j_copy():
        return remote(jsend, jrecv, js_sem, jr_sem, 4)

    def k_copy(k):
        return remote(ksend.at[k], krecv.at[k], ks_sem, kr_sem, k)

    ct_copy = pltpu.make_async_copy(ct_hbm, ct_ref, isem.at[0])
    met_copy = pltpu.make_async_copy(met_hbm, met_ref, isem.at[1])
    ct_copy.start()
    met_copy.start()
    for j in range(2):
        b_copy(j).start()

    barrier = pltpu.get_barrier_semaphore()
    for k in range(1, 8):
        pl.semaphore_signal(barrier, inc=1, device_id=device(k), device_id_type=MESH)

    ct_copy.wait()
    for j, term in enumerate(_split(ct_ref[...])):
        c_ref[j] = term

    met_copy.wait()
    met = met_ref[...]
    low, high = _padq(met[:, :QL]), _padq(met[:, QL:])
    own = jnp.where(a == 0, low, high)
    mx[...] = own
    with jax.named_scope('barrier'):
        pl.semaphore_wait(barrier, 7)

    def m_store(block, row, col):
        for j, term in enumerate(_split(block)):
            m_ref[pl.ds(j * 2 * QP + row, block.shape[0]), pl.ds(col, QP)] = term

    lane = lax.broadcasted_iota(jnp.int32, (GROUP, 128), 1)

    def density_rows():
        ctt[...] = ct_ref[...].T
        rows = ctt[pl.ds(pl.multiple_of(o * ROWS, 8), ROWS), :]
        col = lax.broadcasted_iota(jnp.int32, (ROWS, COLS), 1)
        masked = [jnp.where((col >= d * OCC) & (col < (d + 1) * OCC), rows, 0.0) for d in range(DENS)]
        dens = jnp.dot(jnp.concatenate(masked, axis=0), ct_ref[...], precision=HIGHEST, preferred_element_type=F32)
        dm_ref[...] = jnp.zeros_like(dm_ref)
        for d in range(DENS):
            dm_ref[:, d, :] = dens[d * ROWS:(d + 1) * ROWS]

    def half_transform(g, start, n, with_gamma):
        def body(p, ga):
            m = g * GROUP + 2 * p
            b1, b2, b3 = _split(jnp.concatenate([_padq(b_ref[m]), _padq(b_ref[m + 1])], axis=1))
            terms = [c_ref[j, pl.ds(start, n), :] for j in range(3)]
            if with_gamma:
                extra = _split(dm_ref[pl.ds(m, 2)].reshape(16, L))
                terms = [jnp.concatenate(pair, axis=0) for pair in zip(terms, extra)]
            w = terms[0].shape[0]
            lhs = jnp.concatenate(terms, axis=0)
            r1, r2, r3 = _dot(lhs, b1), _dot(lhs[:2 * w], b2), _dot(lhs[:w], b3)
            h = r1[:w] + ((r1[w:2 * w] + r2[:w]) + (r1[2 * w:] + (r2[w:] + r3)))
            for q in range(2):
                row = pl.multiple_of((2 * p + q) * STRIDE + start, 8)
                for t in range(3):
                    s_ref[t, pl.ds(row, n), :] = h[:n, q * QP + t * 128:q * QP + (t + 1) * 128]
            if with_gamma:
                ga = ga + h[n:n + 8, :QP] + h[n + 8:, QP:]
            return ga

        return body

    def run_half(g, start, n, with_gamma, waits):
        body = half_transform(g, start, n, with_gamma)
        ga = (jnp.zeros((8, QP), F32) if g == 0 else ga_acc[...]) if with_gamma else 0
        for j in range(2):
            if waits and (g == 0 or j == 0):
                b_copy(j if g == 0 else g + 1).wait()
                if g == 0 and j == 1:
                    b_copy(2).start()
                    b_copy(3).start()
            ga = lax.fori_loop(2 * j, 2 * j + 2, lambda p, v: body(2 * p + 1, body(2 * p, v)), ga)
        if with_gamma:
            ga_acc[...] = ga
            if g == GROUPS - 1:
                ga_ref[...] = ga[:DENS]

    def pack(k, g, dst):
        pa, px, pc = peer(k)
        first = (pa * 4 + px * 2 + pc) * MINE

        def load(t, i):
            return s_ref[t, pl.ds(first + i, GROUP, stride=STRIDE), :]

        for i0, n, off, _ in SUBSETS:
            for i in range(n):
                dst[off + i] = load(0, i0 + i).astype(BF16)
                dst[off + n + i] = load(1, i0 + i).astype(BF16)
            at = off + 2 * n
            for j in range(n // 3):
                third = load(2, i0 + 3 * j + 2)
                dst[at + 2 * j] = jnp.where(lane < TAIL, load(2, i0 + 3 * j), pltpu.roll(third, TAIL, 1)).astype(BF16)
                dst[at + 2 * j + 1] = jnp.where(lane < TAIL, load(2, i0 + 3 * j + 1), pltpu.roll(third, 32, 1)).astype(BF16)
            for i in range(n - n % 3, n):
                dst[at + 2 * (n // 3) + i - (n - n % 3)] = load(2, i0 + i).astype(BF16)

    def pack_range(g, k0, k1):
        def body(k, carry):
            pack(k, g, snd.at[k - 1, g])
            return carry

        lax.fori_loop(k0, k1, body, 0)

    def pack_self(g):
        pack(0, g, rcv.at[0, g])
        first = (a * 4 + x * 2 + c) * MINE
        for i in range(MINE):
            for t in range(3):
                _, two, three = _split(s_ref[t, pl.ds(first + i, GROUP, stride=STRIDE), :])
                hl[0, g, i, :, pl.ds(t * 128, 128)] = two
                hl[1, g, i, :, pl.ds(t * 128, 128)] = three

    scope = jax.named_scope
    m_copy(0).start()
    with scope('far'):
        run_half(0, pl.multiple_of((1 - a) * HALFC, 16), HALFC, False, True)
    with scope('packfar'):
        pack_range(0, 4, 8)
    h_send(0, 0, FAR)
    with scope('dens'):
        density_rows()
    with scope('near'):
        run_half(0, pl.multiple_of(a * HALFC, 16), HALFC, True, False)
    with scope('packnear'):
        pack_range(0, 1, 4)
    h_send(0, 0, NEAR)
    pack_self(0)
    with scope('half1'):
        run_half(1, 0, COLS, True, True)
    with scope('m0wait'):
        all_here(mr.at[o], mr_sem.at[0])
    m_copy(1).start()
    m_copy(2).start()
    h_send(0, 1)
    with scope('pack1'):
        pack_range(1, 1, 8)
    pack_self(1)
    with scope('half2'):
        run_half(2, 0, COLS, True, True)
    for k in (4, 6, 2, 5, 7, 3, 1):
        g_copy(k).start()
    h_send(1, 0)
    with scope('m1wait'):
        all_here(mr.at[o], mr_sem.at[1])
    m_copy(3).start()
    with scope('pack2'):
        pack_range(2, 1, 8)
    h_send(2, 0)
    h_send(1, 1)
    h_send(2, 1)
    pack_self(2)

    met = met_ref[...]
    low, high = _padq(met[:, :QL]), _padq(met[:, QL:])
    own = jnp.where(a == 0, low, high)
    oth = jnp.where(a == 0, high, low)
    m_store(own, 0, 0)
    m_store(oth, 0, QP)
    m_store(jnp.pad(oth, ((0, QP - QL), (0, 0))).T, QP, 0)
    with jax.named_scope('m3wait'):
        all_here(mr.at[pl.ds(0, 2)], mr_sem.at[2])
    for q in range(3):
        m_store(mr[q], QP + q * MQ, QP)
    m_store(mr[3][4 * MQ - QL:], QP + 3 * MQ, QP)
    for j in range(3):
        m_ref[pl.ds(j * 2 * QP + QL, QP - QL), :] = jnp.zeros((QP - QL, 2 * QP), BF16)
        m_ref[pl.ds(j * 2 * QP + QP + QL, QP - QL), pl.ds(QP, QP)] = jnp.zeros((QP - QL, QP), BF16)

    def fit(s, g0, g1):
        i0, n, off, _ = SUBSETS[s]

        def half(k, g):
            first = rcv[k, g, pl.ds(off, n)].reshape(n * GROUP, 128)
            second = rcv[k, g, pl.ds(off + n, n)].reshape(n * GROUP, 128)
            at, tails = off + 2 * n, []
            for j in range(n // 3):
                p, q = rcv[k, g, at + 2 * j], rcv[k, g, at + 2 * j + 1]
                third = jnp.where(lane < 128 - TAIL, pltpu.roll(p.astype(F32), 128 - TAIL, 1), pltpu.roll(q.astype(F32), 96, 1))
                tails += [p, q, third.astype(BF16)]
            for i in range(n % 3):
                tails.append(rcv[k, g, at + 2 * (n // 3) + i])
            return jnp.concatenate([first, second, jnp.concatenate(tails, axis=0)], axis=1)

        def fit_group(g, carry):
            with jax.named_scope(f'hwait{s}'):
                all_here(rcv.at[pl.ds(1, 7), g, pl.ds(off, SUBSETS[s][3])], hr_sem.at[g, s])
            lhs = jnp.concatenate([jnp.concatenate([half(k, g), half(k + 4, g)], axis=1) for k in range(4)], axis=0)
            t = _dot(jnp.concatenate([lhs, lhs, lhs], axis=1), m_ref[...])
            h2 = hl[0, g, pl.ds(i0, n)].reshape(n * GROUP, QP)
            h3 = hl[1, g, pl.ds(i0, n)].reshape(n * GROUP, QP)
            ca = _dot(jnp.concatenate([h2, h3], axis=0), m_ref[pl.ds(0, QP), :])
            cb = _dot(h2, m_ref[pl.ds(2 * QP, QP), :])
            w = n * GROUP
            for k in range(4):
                _, px, pc = peer(k)
                part = t[k * w:(k + 1) * w]
                if k == 0:
                    part = part + (ca[:w] + (ca[w:] + cb))
                row = pl.multiple_of((px * 2 + pc) * ROWS + g * GROUP, GROUP)
                t_ref[pl.ds(0, n), pl.ds(row, GROUP), :] = part.reshape(n, GROUP, 2 * QP)
            return carry

        with jax.named_scope(f'fit{s}'):
            lax.fori_loop(g0, g1, fit_group, 0)

    def exchange_subset(s):
        n = SUBSETS[s][1]
        step = 3 if n % 3 == 0 else 2

        def exchange(i, carry):
            terms = zip(*[_split(t_ref[step * i + j]) for j in range(step)])
            t1, t2, t3 = [jnp.concatenate(v, axis=1) for v in terms]
            both = _dot_nt(jnp.concatenate([t1, t2], axis=0), t2)
            kacc[...] += _dot_nt(t1, t1) + both[L:]
            xacc[...] += both[:L] + _dot_nt(t1, t3)
            return carry

        with jax.named_scope(f'exch{s}'):
            lax.fori_loop(0, n // step, exchange, 0)

    kacc[...] = jnp.zeros_like(kacc)
    xacc[...] = jnp.zeros_like(xacc)
    fit(0, 0, 1)

    with jax.named_scope('gwait'):
        all_here(gr_ref.at[pl.ds(1, 7)], gr_sem)
    for g in range(GROUPS):
        h_send(g, 2)
    gam = jnp.concatenate([ga_ref[...] + gr_ref[1] + gr_ref[2] + gr_ref[3],
                           gr_ref[4] + gr_ref[5] + gr_ref[6] + gr_ref[7]], axis=1)
    gam = jnp.concatenate([gam, jnp.zeros_like(gam)], axis=0)

    def stack(v):
        return jnp.concatenate([t.astype(F32) for t in _split(v)], axis=0).astype(BF16)

    def three(v, dot):
        r1, r2, r3 = dot(v, 0), dot(v[:16], 1), dot(v[:8], 2)
        return r1[:8] + ((r1[8:16] + r2[:8]) + (r1[16:] + (r2[8:] + r3)))

    fitted = three(stack(gam), lambda v, j: _dot(v, m_ref[pl.ds(j * 2 * QP, 2 * QP), :]))
    weights = three(stack(fitted), lambda v, j: _dot(v, m_ref[pl.ds(j * 2 * QP, 2 * QP), pl.ds(0, QP)]))
    wf = jnp.concatenate([t.astype(F32) for t in _split(weights)], axis=0)
    for q in range(4):
        blocks = [jnp.zeros((WPAD * q, QP), F32)] if q else []
        wide = jnp.concatenate(blocks + [wf, jnp.zeros((128 - 24 - WPAD * q, QP), F32)], axis=0)
        wt = wide.T.astype(BF16)
        for j in range(3):
            w_ref[pl.ds((3 * q + j) * QP, QP), :] = wt

    def coulomb(p, carry):
        terms = [t for q in range(4) for t in _split(_padq(b_ref[4 * p + q]))]
        r = _dot(jnp.concatenate(terms, axis=1), w_ref[...]).T
        for q in range(4):
            j_ref[4 * p + q] = r[WPAD * q:WPAD * q + 8] + (r[WPAD * q + 8:WPAD * q + 16] + r[WPAD * q + 16:WPAD * q + 24])
        return carry

    with jax.named_scope('coulomb'):
        lax.fori_loop(0, ROWS // 4, coulomb, 0)
    away = []
    for d in range(DENS):
        jd = j_ref[:, d, :]
        jown[d] = jnp.where(a == 0, jd[:, :96], jd[:, 96:])
        away.append(jnp.where(a == 0, jd[:, 96:], jd[:, :96]))
    jsend[...] = jnp.concatenate(away, axis=1)
    j_copy().start()
    for g in range(GROUPS):
        h_send(g, 3)


    fit(0, 1, GROUPS)
    exchange_subset(0)
    for s in range(1, len(SUBSETS)):
        fit(s, 0, GROUPS)
        exchange_subset(s)

    j_copy().wait_recv()
    theirs = jrecv[...]
    for d in range(DENS):
        jown[d] = 2.0 * (jown[d] + theirs[:, 96 * d:96 * (d + 1)])
    kacc[...] += xacc[...] + xacc[...].T
    for k in (7, 6, 5, 4, 3, 2, 1, 0):
        pa, px, pc = peer(k)
        rows = kacc[pl.ds(pl.multiple_of((px * 2 + pc) * ROWS, 8), ROWS), :]
        part = jnp.where(pa == 0, rows[:, :96], rows[:, 96:])
        if k:
            ksend[k] = part
        else:
            krecv[0] = part
    for k in (7, 6, 5, 4, 3, 2, 1):
        k_copy(k).start()
    with jax.named_scope('kwait'):
        all_here(krecv.at[pl.ds(1, 7)], kr_sem)
    for k in (0, 2, 4, 6):
        pa, px, _ = peer(k)
        d = pa * 2 + px
        out_ref[d] = jown[d] - (krecv[k] + krecv[k + 1])

    all_sent(snd, hs_sem)
    all_sent(gr_ref.at[pl.ds(1, 7)], gs_sem)
    all_sent(ksend.at[pl.ds(1, 7)], ks_sem)
    all_sent(mr, ms_sem)
    j_copy().wait_send()


def solution(mesh):
    def local_fock(ints_blk, metric_blk, orbitals):
        bt = jnp.transpose(ints_blk, (1, 2, 0))
        ct = jnp.transpose(orbitals, (0, 2, 1)).reshape(COLS, L)
        ns = len(SUBSETS)
        dma = pltpu.SemaphoreType.DMA
        return pl.pallas_call(
            kernel,
            out_shape=jax.ShapeDtypeStruct((DENS, ROWS, 96), F32),
            in_specs=[pl.BlockSpec(memory_space=pltpu.HBM)] * 3,
            out_specs=pl.BlockSpec(memory_space=pltpu.VMEM),
            scratch_shapes=[
                pltpu.VMEM((ROWS, L, QL), F32),
                pltpu.VMEM((COLS, L), F32),
                pltpu.VMEM((QL, 2 * QL), F32),
                pltpu.VMEM((3, COLS, L), BF16),
                pltpu.VMEM((L, COLS), F32),
                pltpu.VMEM((ROWS, 8, L), F32),
                pltpu.VMEM((3, GROUP * STRIDE, 128), F32),
                pltpu.VMEM((7, GROUPS, SLOTS, GROUP, 128), BF16),
                pltpu.VMEM((8, GROUPS, SLOTS, GROUP, 128), BF16),
                pltpu.VMEM((2, GROUPS, MINE, GROUP, QP), BF16),
                pltpu.VMEM((6 * QP, 2 * QP), BF16),
                pltpu.VMEM((QL, QP), F32),
                pltpu.VMEM((4, MQ, QP), F32),
                pltpu.VMEM((MAXSUB, L, 2 * QP), F32),
                pltpu.VMEM((12 * QP, 128), BF16),
                pltpu.VMEM((8, QP), F32),
                pltpu.VMEM((DENS, QP), F32),
                pltpu.VMEM((8, DENS, QP), F32),
                pltpu.VMEM((ROWS, 8, L), F32),
                pltpu.VMEM((DENS, ROWS, 96), F32),
                pltpu.VMEM((ROWS, DENS * 96), F32),
                pltpu.VMEM((ROWS, DENS * 96), F32),
                pltpu.VMEM((L, L), F32),
                pltpu.VMEM((L, L), F32),
                pltpu.VMEM((8, ROWS, 96), F32),
                pltpu.VMEM((8, ROWS, 96), F32),
                dma((4,)), dma((2,)), dma, dma((GROUPS, ns)), dma, dma((3,)),
                dma, dma, dma, dma, dma, dma,
            ],
            compiler_params=pltpu.CompilerParams(collective_id=0, has_side_effects=True, vmem_limit_bytes=56_360_000),
            cost_estimate=pl.CostEstimate(flops=25_000_000_000, bytes_accessed=16_000_000, transcendentals=0),
        )(bt, ct, metric_blk)

    return jax.shard_map(local_fock, mesh=mesh, in_specs=(P(('sys', 'aux'), 'orb', None), P(('sys', 'aux'), None), P('sys', None, None)), out_specs=P('sys', 'orb', 'aux'), check_vma=False)
```

```python
import functools

import jax
import jax.numpy as jnp
from jax import lax
from jax.experimental import pallas as pl
from jax.experimental.pallas import tpu as pltpu
from jax.sharding import PartitionSpec as P

MESH = pl.DeviceIdType.MESH
F32, BF16 = jnp.float32, jnp.bfloat16
HIGHEST = lax.Precision.HIGHEST

DENS, L, OCC = 4, 192, 40
COLS = DENS * OCC
MINE = COLS // 8
ROWS = 48
GROUP = 16
GROUPS = ROWS // GROUP
QL, QP = 336, 384
TAIL = QL - 256
STRIDE = 168
HALFC = COLS // 2
MQ = 88
WPAD = 32
NT = (((1,), (1,)), ((), ()))


def _subsets(sizes):
    out, first, off = [], 0, 0
    for n in sizes:
        r = n % 8
        tails = 5 * (n // 8) + 2 * (r // 3) + r % 3
        out.append((first, n, off, 2 * n + tails))
        first, off = first + n, off + 2 * n + tails
    return out, off


SUBSETS, SLOTS = _subsets((8, 8, 3, 1))
MAXSUB = max(s[1] for s in SUBSETS)


def _split(v):
    one = v.astype(BF16)
    rest = v - one.astype(F32)
    two = rest.astype(BF16)
    return one, two, (rest - two.astype(F32)).astype(BF16)


def _dot(p, q):
    return jnp.dot(p, q, preferred_element_type=F32)


def _dot_nt(p, q):
    return lax.dot_general(p, q, NT, preferred_element_type=F32)


def _padq(v):
    return jnp.pad(v, ((0, 0), (0, QP - QL)))


def kernel(b_hbm, ct_hbm, met_hbm, out_ref,
           b_ref, ct_ref, met_ref, c_ref, ctt, dm_ref, s_ref, snd, rcv, hl, m_ref, mx, mr, t_ref, w_ref,
           ga_acc, ga_ref, gr_ref, j_ref, jown, jsend, jrecv, kacc, xacc, ksend, krecv,
           bsem, isem, hs_sem, hr_sem, ms_sem, mr_sem, gs_sem, gr_sem, js_sem, jr_sem, ks_sem, kr_sem):
    a = lax.axis_index('aux')
    o = lax.axis_index('orb')
    x, c = o // 2, o % 2
    sys = lax.axis_index('sys')

    def peer(k):
        return (a + k // 4) % 2, (x + (k // 2) % 2) % 2, (c + k % 2) % 2

    def device(k):
        pa, px, pc = peer(k)
        return (sys, pa, px * 2 + pc)

    def remote(src, dst, ssem, rsem, k):
        return pltpu.make_async_remote_copy(src_ref=src, dst_ref=dst, send_sem=ssem, recv_sem=rsem,
                                            device_id=device(k), device_id_type=MESH)

    def b_copy(j):
        first, n = ((0, 8), (8, 8), (16, 16), (32, 16))[j]
        return pltpu.make_async_copy(b_hbm.at[pl.ds(first, n)], b_ref.at[pl.ds(first, n)], bsem.at[j])

    def all_sent(ref, sem):
        remote(ref, ref, sem, sem, 0).wait_send()

    def all_here(ref, sem):
        remote(ref, ref, sem, sem, 0).wait_recv()

    def h_copy(k, g, s):
        _, _, off, n = SUBSETS[s]
        return remote(snd.at[k - 1, g, pl.ds(off, n)], rcv.at[k, g, pl.ds(off, n)],
                      hs_sem, hr_sem.at[g, s], k)

    FAR, NEAR = (4, 6, 5, 7), (2, 3, 1)

    def h_send(g, s, ks=(4, 6, 2, 5, 7, 3, 1)):
        for k in ks:
            h_copy(k, g, s).start()

    def m_copy(step):
        mine = o if step < 3 else (1 - x) * 2 + c
        src = mx.at[pl.ds(pl.multiple_of(o * MQ - (o // 3) * (4 * MQ - QL), 8), MQ)] if step == 0 else mr.at[mine]
        return remote(src, mr.at[mine], ms_sem, mr_sem.at[min(step, 2)], (4, 2, 1, 1)[step])

    def g_copy(k):
        return remote(ga_ref, gr_ref.at[k], gs_sem, gr_sem, k)

    def j_copy():
        return remote(jsend, jrecv, js_sem, jr_sem, 4)

    def k_copy(k):
        return remote(ksend.at[k], krecv.at[k], ks_sem, kr_sem, k)

    ct_copy = pltpu.make_async_copy(ct_hbm, ct_ref, isem.at[0])
    met_copy = pltpu.make_async_copy(met_hbm, met_ref, isem.at[1])
    ct_copy.start()
    met_copy.start()
    for j in range(2):
        b_copy(j).start()

    barrier = pltpu.get_barrier_semaphore()
    for k in range(1, 8):
        pl.semaphore_signal(barrier, inc=1, device_id=device(k), device_id_type=MESH)

    ct_copy.wait()
    for j, term in enumerate(_split(ct_ref[...])):
        c_ref[j] = term

    met_copy.wait()
    met = met_ref[...]
    low, high = _padq(met[:, :QL]), _padq(met[:, QL:])
    own = jnp.where(a == 0, low, high)
    mx[...] = own
    with jax.named_scope('barrier'):
        pl.semaphore_wait(barrier, 7)

    def m_store(block, row, col):
        for j, term in enumerate(_split(block)):
            m_ref[pl.ds(j * 2 * QP + row, block.shape[0]), pl.ds(col, QP)] = term

    lane = lax.broadcasted_iota(jnp.int32, (GROUP, 128), 1)

    def density_rows():
        ctt[...] = ct_ref[...].T
        rows = ctt[pl.ds(pl.multiple_of(o * ROWS, 8), ROWS), :]
        col = lax.broadcasted_iota(jnp.int32, (ROWS, COLS), 1)
        masked = [jnp.where((col >= d * OCC) & (col < (d + 1) * OCC), rows, 0.0) for d in range(DENS)]
        dens = jnp.dot(jnp.concatenate(masked, axis=0), ct_ref[...], precision=HIGHEST, preferred_element_type=F32)
        dm_ref[...] = jnp.zeros_like(dm_ref)
        for d in range(DENS):
            dm_ref[:, d, :] = dens[d * ROWS:(d + 1) * ROWS]

    def half_transform(g, start, n, with_gamma):
        def body(p, ga):
            m = g * GROUP + 2 * p
            b1, b2, b3 = _split(jnp.concatenate([_padq(b_ref[m]), _padq(b_ref[m + 1])], axis=1))
            terms = [c_ref[j, pl.ds(start, n), :] for j in range(3)]
            if with_gamma:
                extra = _split(dm_ref[pl.ds(m, 2)].reshape(16, L))
                terms = [jnp.concatenate(pair, axis=0) for pair in zip(terms, extra)]
            w = terms[0].shape[0]
            lhs = jnp.concatenate(terms, axis=0)
            r1, r2, r3 = _dot(lhs, b1), _dot(lhs[:2 * w], b2), _dot(lhs[:w], b3)
            h = r1[:w] + ((r1[w:2 * w] + r2[:w]) + (r1[2 * w:] + (r2[w:] + r3)))
            for q in range(2):
                row = pl.multiple_of((2 * p + q) * STRIDE + start, 8)
                for t in range(3):
                    s_ref[t, pl.ds(row, n), :] = h[:n, q * QP + t * 128:q * QP + (t + 1) * 128]
            if with_gamma:
                ga = ga + h[n:n + 8, :QP] + h[n + 8:, QP:]
            return ga

        return body

    def run_half(g, start, n, with_gamma, waits):
        body = half_transform(g, start, n, with_gamma)
        ga = (jnp.zeros((8, QP), F32) if g == 0 else ga_acc[...]) if with_gamma else 0
        for j in range(2):
            if waits and (g == 0 or j == 0):
                b_copy(j if g == 0 else g + 1).wait()
                if g == 0 and j == 1:
                    b_copy(2).start()
                    b_copy(3).start()
            ga = lax.fori_loop(2 * j, 2 * j + 2, lambda p, v: body(2 * p + 1, body(2 * p, v)), ga)
        if with_gamma:
            ga_acc[...] = ga
            if g == GROUPS - 1:
                ga_ref[...] = ga[:DENS]

    def pack(k, g, dst):
        pa, px, pc = peer(k)
        first = (pa * 4 + px * 2 + pc) * MINE

        def load(t, i):
            return s_ref[t, pl.ds(first + i, GROUP, stride=STRIDE), :]

        for i0, n, off, _ in SUBSETS:
            for i in range(n):
                dst[off + i] = load(0, i0 + i).astype(BF16)
                dst[off + n + i] = load(1, i0 + i).astype(BF16)
            at, i = off + 2 * n, i0
            while i < i0 + n:
                if i0 + n - i >= 8:
                    v = [load(2, i + j) for j in range(8)]
                    roll = lambda j, by: pltpu.roll(v[j], by, 1)
                    free = [roll(5, 80), jnp.where(lane < 112, roll(5, 32), roll(7, 64)), roll(6, 80),
                            jnp.where(lane < 112, roll(6, 32), roll(7, 48)), roll(7, 80)]
                    i += 8
                elif i0 + n - i >= 3:
                    v = [load(2, i + j) for j in range(3)]
                    free = [pltpu.roll(v[2], 80, 1), pltpu.roll(v[2], 32, 1)]
                    i += 3
                else:
                    v, free = [load(2, i)], None
                    i += 1
                for j in range(len(free) if free else 1):
                    dst[at] = (jnp.where(lane < TAIL, v[j], free[j]) if free else v[j]).astype(BF16)
                    at += 1

    def pack_range(g, k0, k1):
        def body(k, carry):
            pack(k, g, snd.at[k - 1, g])
            return carry

        lax.fori_loop(k0, k1, body, 0)

    def pack_self(g):
        pack(0, g, rcv.at[0, g])
        first = (a * 4 + x * 2 + c) * MINE
        for i in range(MINE):
            for t in range(3):
                _, two, three = _split(s_ref[t, pl.ds(first + i, GROUP, stride=STRIDE), :])
                hl[0, g, i, :, pl.ds(t * 128, 128)] = two
                hl[1, g, i, :, pl.ds(t * 128, 128)] = three

    scope = jax.named_scope
    m_copy(0).start()
    with scope('far'):
        run_half(0, pl.multiple_of((1 - a) * HALFC, 16), HALFC, False, True)
    with scope('packfar'):
        pack_range(0, 4, 8)
    h_send(0, 0, FAR)
    with scope('dens'):
        density_rows()
    with scope('near'):
        run_half(0, pl.multiple_of(a * HALFC, 16), HALFC, True, False)
    with scope('packnear'):
        pack_range(0, 1, 4)
    h_send(0, 0, NEAR)
    h_send(0, 1, (4, 5))
    pack_self(0)
    with scope('half1'):
        run_half(1, 0, COLS, True, True)
    with scope('m0wait'):
        all_here(mr.at[o], mr_sem.at[0])
    m_copy(1).start()
    m_copy(2).start()
    h_send(0, 1, (6, 2, 7, 3, 1))
    with scope('pack1'):
        pack_range(1, 1, 8)
    pack_self(1)
    with scope('half2'):
        run_half(2, 0, COLS, True, True)
    for k in (4, 6, 2, 5, 7, 3, 1):
        g_copy(k).start()
    h_send(1, 0)
    with scope('pack2'):
        pack_range(2, 1, 8)
    h_send(2, 0)
    h_send(1, 1)
    h_send(2, 1)
    pack_self(2)
    with scope('m1wait'):
        all_here(mr.at[o], mr_sem.at[1])
    m_copy(3).start()

    met = met_ref[...]
    low, high = _padq(met[:, :QL]), _padq(met[:, QL:])
    own = jnp.where(a == 0, low, high)
    oth = jnp.where(a == 0, high, low)
    m_store(own, 0, 0)
    m_store(oth, 0, QP)
    m_store(jnp.pad(oth, ((0, QP - QL), (0, 0))).T, QP, 0)
    with jax.named_scope('m3wait'):
        all_here(mr.at[pl.ds(0, 2)], mr_sem.at[2])
    for q in range(3):
        m_store(mr[q], QP + q * MQ, QP)
    m_store(mr[3][4 * MQ - QL:], QP + 3 * MQ, QP)
    for j in range(3):
        m_ref[pl.ds(j * 2 * QP + QL, QP - QL), :] = jnp.zeros((QP - QL, 2 * QP), BF16)
        m_ref[pl.ds(j * 2 * QP + QP + QL, QP - QL), pl.ds(QP, QP)] = jnp.zeros((QP - QL, QP), BF16)

    def fit(s, g0, g1):
        i0, n, off, _ = SUBSETS[s]

        def half(k, g):
            first = rcv[k, g, pl.ds(off, n)].reshape(n * GROUP, 128)
            second = rcv[k, g, pl.ds(off + n, n)].reshape(n * GROUP, 128)
            at, tails, left = off + 2 * n, [], n
            roll = lambda v, by: pltpu.roll(v.astype(F32), by, 1)
            while left:
                if left >= 8:
                    v = [rcv[k, g, at + j] for j in range(5)]
                    late = [jnp.where(lane < 48, roll(v[0], 48), roll(v[1], 96)), jnp.where(lane < 48, roll(v[2], 48), roll(v[3], 96)),
                            jnp.where(lane < 48, roll(v[4], 48), jnp.where(lane < 64, roll(v[1], 64), roll(v[3], 80)))]
                    left -= 8
                elif left >= 3:
                    v = [rcv[k, g, at + j] for j in range(2)]
                    late = [jnp.where(lane < 48, roll(v[0], 48), roll(v[1], 96))]
                    left -= 3
                else:
                    v, late = [rcv[k, g, at]], []
                    left -= 1
                tails += v + [w.astype(BF16) for w in late]
                at += len(v)
            return jnp.concatenate([first, second, jnp.concatenate(tails, axis=0)], axis=1)

        def fit_group(g, carry):
            with jax.named_scope(f'hwait{s}'):
                all_here(rcv.at[pl.ds(1, 7), g, pl.ds(off, SUBSETS[s][3])], hr_sem.at[g, s])
            lhs = jnp.concatenate([jnp.concatenate([half(k, g), half(k + 4, g)], axis=1) for k in range(4)], axis=0)
            t = _dot(jnp.concatenate([lhs, lhs, lhs], axis=1), m_ref[...])
            h2 = hl[0, g, pl.ds(i0, n)].reshape(n * GROUP, QP)
            h3 = hl[1, g, pl.ds(i0, n)].reshape(n * GROUP, QP)
            ca = _dot(jnp.concatenate([h2, h3], axis=0), m_ref[pl.ds(0, QP), :])
            cb = _dot(h2, m_ref[pl.ds(2 * QP, QP), :])
            w = n * GROUP
            for k in range(4):
                _, px, pc = peer(k)
                part = t[k * w:(k + 1) * w]
                if k == 0:
                    part = part + (ca[:w] + (ca[w:] + cb))
                row = pl.multiple_of((px * 2 + pc) * ROWS + g * GROUP, GROUP)
                t_ref[pl.ds(0, n), pl.ds(row, GROUP), :] = part.reshape(n, GROUP, 2 * QP)
            return carry

        with jax.named_scope(f'fit{s}'):
            lax.fori_loop(g0, g1, fit_group, 0)

    def exchange_subset(s):
        n = SUBSETS[s][1]
        step = 4 if n % 4 == 0 else n

        def exchange(i, carry):
            terms = zip(*[_split(t_ref[step * i + j]) for j in range(step)])
            t1, t2, t3 = [jnp.concatenate(v, axis=1) for v in terms]
            both = _dot_nt(jnp.concatenate([t1, t2], axis=0), t2)
            kacc[...] += _dot_nt(t1, t1) + both[L:]
            xacc[...] += both[:L] + _dot_nt(t1, t3)
            return carry

        with jax.named_scope(f'exch{s}'):
            lax.fori_loop(0, n // step, exchange, 0)

    kacc[...] = jnp.zeros_like(kacc)
    xacc[...] = jnp.zeros_like(xacc)
    fit(0, 0, 1)

    with jax.named_scope('gwait'):
        all_here(gr_ref.at[pl.ds(1, 7)], gr_sem)
    for g in range(GROUPS):
        h_send(g, 2)
    gam = jnp.concatenate([ga_ref[...] + gr_ref[1] + gr_ref[2] + gr_ref[3],
                           gr_ref[4] + gr_ref[5] + gr_ref[6] + gr_ref[7]], axis=1)
    gam = jnp.concatenate([gam, jnp.zeros_like(gam)], axis=0)

    def stack(v):
        return jnp.concatenate([t.astype(F32) for t in _split(v)], axis=0).astype(BF16)

    def three(v, dot):
        r1, r2, r3 = dot(v, 0), dot(v[:16], 1), dot(v[:8], 2)
        return r1[:8] + ((r1[8:16] + r2[:8]) + (r1[16:] + (r2[8:] + r3)))

    fitted = three(stack(gam), lambda v, j: _dot(v, m_ref[pl.ds(j * 2 * QP, 2 * QP), :]))
    weights = three(stack(fitted), lambda v, j: _dot(v, m_ref[pl.ds(j * 2 * QP, 2 * QP), pl.ds(0, QP)]))
    wf = jnp.concatenate([t.astype(F32) for t in _split(weights)], axis=0)
    for q in range(4):
        blocks = [jnp.zeros((WPAD * q, QP), F32)] if q else []
        wide = jnp.concatenate(blocks + [wf, jnp.zeros((128 - 24 - WPAD * q, QP), F32)], axis=0)
        wt = wide.T.astype(BF16)
        for j in range(3):
            w_ref[pl.ds((3 * q + j) * QP, QP), :] = wt

    def coulomb(p, carry):
        terms = [t for q in range(4) for t in _split(_padq(b_ref[4 * p + q]))]
        r = _dot(jnp.concatenate(terms, axis=1), w_ref[...]).T
        for q in range(4):
            j_ref[4 * p + q] = r[WPAD * q:WPAD * q + 8] + (r[WPAD * q + 8:WPAD * q + 16] + r[WPAD * q + 16:WPAD * q + 24])
        return carry

    with jax.named_scope('coulomb'):
        lax.fori_loop(0, ROWS // 4, coulomb, 0)
    away = []
    for d in range(DENS):
        jd = j_ref[:, d, :]
        jown[d] = jnp.where(a == 0, jd[:, :96], jd[:, 96:])
        away.append(jnp.where(a == 0, jd[:, 96:], jd[:, :96]))
    jsend[...] = jnp.concatenate(away, axis=1)
    for g in range(GROUPS):
        h_send(g, 3)
    j_copy().start()


    fit(0, 1, GROUPS)
    exchange_subset(0)
    for s in range(1, len(SUBSETS)):
        fit(s, 0, GROUPS)
        exchange_subset(s)

    j_copy().wait_recv()
    theirs = jrecv[...]
    for d in range(DENS):
        jown[d] = 2.0 * (jown[d] + theirs[:, 96 * d:96 * (d + 1)])
    kacc[...] += xacc[...] + xacc[...].T
    for k in (7, 6, 5, 4, 3, 2, 1, 0):
        pa, px, pc = peer(k)
        rows = kacc[pl.ds(pl.multiple_of((px * 2 + pc) * ROWS, 8), ROWS), :]
        part = jnp.where(pa == 0, rows[:, :96], rows[:, 96:])
        if k:
            ksend[k] = part
        else:
            krecv[0] = part
    for k in (7, 6, 5, 4, 3, 2, 1):
        k_copy(k).start()
    with jax.named_scope('kwait'):
        all_here(krecv.at[pl.ds(1, 7)], kr_sem)
    for k in (0, 2, 4, 6):
        pa, px, _ = peer(k)
        d = pa * 2 + px
        out_ref[d] = jown[d] - (krecv[k] + krecv[k + 1])

    all_sent(snd, hs_sem)
    all_sent(gr_ref.at[pl.ds(1, 7)], gs_sem)
    all_sent(ksend.at[pl.ds(1, 7)], ks_sem)
    all_sent(mr, ms_sem)
    j_copy().wait_send()


def solution(mesh):
    def local_fock(ints_blk, metric_blk, orbitals):
        bt = jnp.transpose(ints_blk, (1, 2, 0))
        ct = jnp.transpose(orbitals, (0, 2, 1)).reshape(COLS, L)
        ns = len(SUBSETS)
        dma = pltpu.SemaphoreType.DMA
        return pl.pallas_call(
            kernel,
            out_shape=jax.ShapeDtypeStruct((DENS, ROWS, 96), F32),
            in_specs=[pl.BlockSpec(memory_space=pltpu.HBM)] * 3,
            out_specs=pl.BlockSpec(memory_space=pltpu.VMEM),
            scratch_shapes=[
                pltpu.VMEM((ROWS, L, QL), F32),
                pltpu.VMEM((COLS, L), F32),
                pltpu.VMEM((QL, 2 * QL), F32),
                pltpu.VMEM((3, COLS, L), BF16),
                pltpu.VMEM((L, COLS), F32),
                pltpu.VMEM((ROWS, 8, L), F32),
                pltpu.VMEM((3, GROUP * STRIDE, 128), F32),
                pltpu.VMEM((7, GROUPS, SLOTS, GROUP, 128), BF16),
                pltpu.VMEM((8, GROUPS, SLOTS, GROUP, 128), BF16),
                pltpu.VMEM((2, GROUPS, MINE, GROUP, QP), BF16),
                pltpu.VMEM((6 * QP, 2 * QP), BF16),
                pltpu.VMEM((QL, QP), F32),
                pltpu.VMEM((4, MQ, QP), F32),
                pltpu.VMEM((MAXSUB, L, 2 * QP), F32),
                pltpu.VMEM((12 * QP, 128), BF16),
                pltpu.VMEM((8, QP), F32),
                pltpu.VMEM((DENS, QP), F32),
                pltpu.VMEM((8, DENS, QP), F32),
                pltpu.VMEM((ROWS, 8, L), F32),
                pltpu.VMEM((DENS, ROWS, 96), F32),
                pltpu.VMEM((ROWS, DENS * 96), F32),
                pltpu.VMEM((ROWS, DENS * 96), F32),
                pltpu.VMEM((L, L), F32),
                pltpu.VMEM((L, L), F32),
                pltpu.VMEM((8, ROWS, 96), F32),
                pltpu.VMEM((8, ROWS, 96), F32),
                dma((4,)), dma((2,)), dma, dma((GROUPS, ns)), dma, dma((3,)),
                dma, dma, dma, dma, dma, dma,
            ],
            compiler_params=pltpu.CompilerParams(collective_id=0, has_side_effects=True, vmem_limit_bytes=56_360_000),
            cost_estimate=pl.CostEstimate(flops=25_000_000_000, bytes_accessed=16_000_000, transcendentals=0),
        )(bt, ct, metric_blk)

    return jax.shard_map(local_fock, mesh=mesh, in_specs=(P(('sys', 'aux'), 'orb', None), P(('sys', 'aux'), None), P('sys', None, None)), out_specs=P('sys', 'orb', 'aux'), check_vma=False)
```

```python
import functools

import jax
import jax.numpy as jnp
from jax import lax
from jax.experimental import pallas as pl
from jax.experimental.pallas import tpu as pltpu
from jax.sharding import PartitionSpec as P

MESH = pl.DeviceIdType.MESH
F32, BF16 = jnp.float32, jnp.bfloat16
HIGHEST = lax.Precision.HIGHEST

DENS, L, OCC = 4, 192, 40
COLS = DENS * OCC
MINE = COLS // 8
ROWS = 48
GROUP = 16
GROUPS = ROWS // GROUP
QL, QP = 336, 384
TAIL = QL - 256
STRIDE = 168
HALFC = COLS // 2
MQ = 88
WPAD = 32
NT = (((1,), (1,)), ((), ()))


def _subsets(sizes):
    out, first, off = [], 0, 0
    for n in sizes:
        r = n % 8
        tails = 5 * (n // 8) + 2 * (r // 3) + r % 3
        out.append((first, n, off, 2 * n + tails))
        first, off = first + n, off + 2 * n + tails
    return out, off


SUBSETS, SLOTS = _subsets((8, 8, 3, 1))
MAXSUB = max(s[1] for s in SUBSETS)


def _split(v):
    one = v.astype(BF16)
    rest = v - one.astype(F32)
    two = rest.astype(BF16)
    return one, two, (rest - two.astype(F32)).astype(BF16)


def _dot(p, q):
    return jnp.dot(p, q, preferred_element_type=F32)


def _dot_nt(p, q):
    return lax.dot_general(p, q, NT, preferred_element_type=F32)


def _padq(v):
    return jnp.pad(v, ((0, 0), (0, QP - QL)))


def kernel(b_hbm, ct_hbm, met_hbm, out_ref,
           b_ref, ct_ref, met_ref, c_ref, ctt, dm_ref, s_ref, snd, rcv, hl, m_ref, mx, mr, t_ref, w_ref,
           ga_acc, ga_ref, gr_ref, j_ref, jown, jsend, jrecv, kacc, xacc, ksend, krecv,
           bsem, isem, hs_sem, hr_sem, ms_sem, mr_sem, gs_sem, gr_sem, js_sem, jr_sem, ks_sem, kr_sem):
    a = lax.axis_index('aux')
    o = lax.axis_index('orb')
    x, c = o // 2, o % 2
    sys = lax.axis_index('sys')

    def peer(k):
        return (a + k // 4) % 2, (x + (k // 2) % 2) % 2, (c + k % 2) % 2

    def device(k):
        pa, px, pc = peer(k)
        return (sys, pa, px * 2 + pc)

    def remote(src, dst, ssem, rsem, k):
        return pltpu.make_async_remote_copy(src_ref=src, dst_ref=dst, send_sem=ssem, recv_sem=rsem,
                                            device_id=device(k), device_id_type=MESH)

    def b_copy(j):
        first, n = ((0, 8), (8, 8), (16, 16), (32, 16))[j]
        return pltpu.make_async_copy(b_hbm.at[pl.ds(first, n)], b_ref.at[pl.ds(first, n)], bsem.at[j])

    def all_sent(ref, sem):
        remote(ref, ref, sem, sem, 0).wait_send()

    def all_here(ref, sem):
        remote(ref, ref, sem, sem, 0).wait_recv()

    def h_copy(k, g, s):
        _, _, off, n = SUBSETS[s]
        return remote(snd.at[k - 1, g, pl.ds(off, n)], rcv.at[k, g, pl.ds(off, n)],
                      hs_sem, hr_sem.at[g, s], k)

    FAR, NEAR = (4, 6, 5, 7), (2, 3, 1)

    def h_send(g, s, ks=(4, 6, 2, 5, 7, 3, 1)):
        for k in ks:
            h_copy(k, g, s).start()

    def m_copy(step):
        mine = o if step != 3 else (1 - x) * 2 + c
        src = mx.at[pl.ds(pl.multiple_of(o * MQ - (o // 3) * (4 * MQ - QL), 8), MQ)] if step in (0, 4) else mr.at[mine]
        return remote(src, mr.at[mine], ms_sem, mr_sem.at[(0, 1, 2, 2, 1)[step]], (4, 2, 1, 1, 6)[step])

    def g_copy(k):
        return remote(ga_ref, gr_ref.at[k], gs_sem, gr_sem, k)

    def j_copy():
        return remote(jsend, jrecv, js_sem, jr_sem, 4)

    def k_copy(k):
        return remote(ksend.at[k], krecv.at[k], ks_sem, kr_sem, k)

    ct_copy = pltpu.make_async_copy(ct_hbm, ct_ref, isem.at[0])
    met_copy = pltpu.make_async_copy(met_hbm, met_ref, isem.at[1])
    ct_copy.start()
    met_copy.start()
    for j in range(2):
        b_copy(j).start()

    barrier = pltpu.get_barrier_semaphore()
    for k in range(1, 8):
        pl.semaphore_signal(barrier, inc=1, device_id=device(k), device_id_type=MESH)

    ct_copy.wait()
    for j, term in enumerate(_split(ct_ref[...])):
        c_ref[j] = term

    met_copy.wait()
    met = met_ref[...]
    low, high = _padq(met[:, :QL]), _padq(met[:, QL:])
    own = jnp.where(a == 0, low, high)
    mx[...] = own
    with jax.named_scope('barrier'):
        pl.semaphore_wait(barrier, 7)

    def m_store(block, row, col):
        for j, term in enumerate(_split(block)):
            m_ref[pl.ds(j * 2 * QP + row, block.shape[0]), pl.ds(col, QP)] = term

    lane = lax.broadcasted_iota(jnp.int32, (GROUP, 128), 1)

    def density_rows():
        ctt[...] = ct_ref[...].T
        rows = ctt[pl.ds(pl.multiple_of(o * ROWS, 8), ROWS), :]
        col = lax.broadcasted_iota(jnp.int32, (ROWS, COLS), 1)
        masked = [jnp.where((col >= d * OCC) & (col < (d + 1) * OCC), rows, 0.0) for d in range(DENS)]
        dens = jnp.dot(jnp.concatenate(masked, axis=0), ct_ref[...], precision=HIGHEST, preferred_element_type=F32)
        dm_ref[...] = jnp.zeros_like(dm_ref)
        for d in range(DENS):
            dm_ref[:, d, :] = dens[d * ROWS:(d + 1) * ROWS]

    def half_transform(g, start, n, with_gamma):
        def body(p, ga):
            m = g * GROUP + 2 * p
            b1, b2, b3 = _split(jnp.concatenate([_padq(b_ref[m]), _padq(b_ref[m + 1])], axis=1))
            terms = [c_ref[j, pl.ds(start, n), :] for j in range(3)]
            if with_gamma:
                extra = _split(dm_ref[pl.ds(m, 2)].reshape(16, L))
                terms = [jnp.concatenate(pair, axis=0) for pair in zip(terms, extra)]
            w = terms[0].shape[0]
            lhs = jnp.concatenate(terms, axis=0)
            r1, r2, r3 = _dot(lhs, b1), _dot(lhs[:2 * w], b2), _dot(lhs[:w], b3)
            h = r1[:w] + ((r1[w:2 * w] + r2[:w]) + (r1[2 * w:] + (r2[w:] + r3)))
            for q in range(2):
                row = pl.multiple_of((2 * p + q) * STRIDE + start, 8)
                for t in range(3):
                    s_ref[t, pl.ds(row, n), :] = h[:n, q * QP + t * 128:q * QP + (t + 1) * 128]
            if with_gamma:
                ga = ga + h[n:n + 8, :QP] + h[n + 8:, QP:]
            return ga

        return body

    def run_half(g, start, n, with_gamma, waits):
        body = half_transform(g, start, n, with_gamma)
        ga = (jnp.zeros((8, QP), F32) if g == 0 else ga_acc[...]) if with_gamma else 0
        for j in range(2):
            if waits and (g == 0 or j == 0):
                b_copy(j if g == 0 else g + 1).wait()
                if g == 0 and j == 1:
                    b_copy(2).start()
                    b_copy(3).start()
            ga = lax.fori_loop(2 * j, 2 * j + 2, lambda p, v: body(2 * p + 1, body(2 * p, v)), ga)
        if with_gamma:
            ga_acc[...] = ga
            if g == GROUPS - 1:
                ga_ref[...] = ga[:DENS]

    def pack(k, g, dst):
        pa, px, pc = peer(k)
        first = (pa * 4 + px * 2 + pc) * MINE

        def load(t, i):
            return s_ref[t, pl.ds(first + i, GROUP, stride=STRIDE), :]

        for i0, n, off, _ in SUBSETS:
            for i in range(n):
                dst[off + i] = load(0, i0 + i).astype(BF16)
                dst[off + n + i] = load(1, i0 + i).astype(BF16)
            at, i = off + 2 * n, i0
            while i < i0 + n:
                if i0 + n - i >= 8:
                    v = [load(2, i + j) for j in range(8)]
                    roll = lambda j, by: pltpu.roll(v[j], by, 1)
                    free = [roll(5, 80), jnp.where(lane < 112, roll(5, 32), roll(7, 64)), roll(6, 80),
                            jnp.where(lane < 112, roll(6, 32), roll(7, 48)), roll(7, 80)]
                    i += 8
                elif i0 + n - i >= 3:
                    v = [load(2, i + j) for j in range(3)]
                    free = [pltpu.roll(v[2], 80, 1), pltpu.roll(v[2], 32, 1)]
                    i += 3
                else:
                    v, free = [load(2, i)], None
                    i += 1
                for j in range(len(free) if free else 1):
                    dst[at] = (jnp.where(lane < TAIL, v[j], free[j]) if free else v[j]).astype(BF16)
                    at += 1

    def pack_range(g, k0, k1):
        def body(k, carry):
            pack(k, g, snd.at[k - 1, g])
            return carry

        lax.fori_loop(k0, k1, body, 0)

    def pack_self(g):
        pack(0, g, rcv.at[0, g])
        first = (a * 4 + x * 2 + c) * MINE
        for i in range(MINE):
            for t in range(3):
                _, two, three = _split(s_ref[t, pl.ds(first + i, GROUP, stride=STRIDE), :])
                hl[0, g, i, :, pl.ds(t * 128, 128)] = two
                hl[1, g, i, :, pl.ds(t * 128, 128)] = three

    scope = jax.named_scope
    m_copy(0).start()
    pl.when(c == 1)(lambda: m_copy(4).start())
    with scope('far'):
        run_half(0, pl.multiple_of((1 - a) * HALFC, 16), HALFC, False, True)
    with scope('packfar'):
        pack_range(0, 4, 8)
    h_send(0, 0, FAR)
    with scope('dens'):
        density_rows()
    with scope('near'):
        run_half(0, pl.multiple_of(a * HALFC, 16), HALFC, True, False)
    with scope('packnear'):
        pack_range(0, 1, 4)
    h_send(0, 0, NEAR)
    h_send(0, 1, (4, 5))
    pack_self(0)
    with scope('half1'):
        run_half(1, 0, COLS, True, True)
    with scope('m0wait'):
        all_here(mr.at[o], mr_sem.at[0])
    pl.when(c == 0)(lambda: m_copy(1).start())
    m_copy(2).start()
    h_send(0, 1, (6, 2, 7, 3, 1))
    with scope('pack1'):
        pack_range(1, 1, 8)
    pack_self(1)
    with scope('half2'):
        run_half(2, 0, COLS, True, True)
    for k in (4, 6, 2, 5, 7, 3, 1):
        g_copy(k).start()
    h_send(1, 0)
    with scope('pack2'):
        pack_range(2, 1, 8)
    h_send(2, 0)
    h_send(1, 1)
    h_send(2, 1)
    pack_self(2)
    with scope('m1wait'):
        all_here(mr.at[o], mr_sem.at[1])
    m_copy(3).start()

    met = met_ref[...]
    low, high = _padq(met[:, :QL]), _padq(met[:, QL:])
    own = jnp.where(a == 0, low, high)
    oth = jnp.where(a == 0, high, low)
    m_store(own, 0, 0)
    m_store(oth, 0, QP)
    m_store(jnp.pad(oth, ((0, QP - QL), (0, 0))).T, QP, 0)
    with jax.named_scope('m3wait'):
        all_here(mr.at[pl.ds(0, 2)], mr_sem.at[2])
    for q in range(3):
        m_store(mr[q], QP + q * MQ, QP)
    m_store(mr[3][4 * MQ - QL:], QP + 3 * MQ, QP)
    for j in range(3):
        m_ref[pl.ds(j * 2 * QP + QL, QP - QL), :] = jnp.zeros((QP - QL, 2 * QP), BF16)
        m_ref[pl.ds(j * 2 * QP + QP + QL, QP - QL), pl.ds(QP, QP)] = jnp.zeros((QP - QL, QP), BF16)

    def fit(s, g0, g1):
        i0, n, off, _ = SUBSETS[s]

        def half(k, g):
            first = rcv[k, g, pl.ds(off, n)].reshape(n * GROUP, 128)
            second = rcv[k, g, pl.ds(off + n, n)].reshape(n * GROUP, 128)
            at, tails, left = off + 2 * n, [], n
            roll = lambda v, by: pltpu.roll(v.astype(F32), by, 1)
            while left:
                if left >= 8:
                    v = [rcv[k, g, at + j] for j in range(5)]
                    late = [jnp.where(lane < 48, roll(v[0], 48), roll(v[1], 96)), jnp.where(lane < 48, roll(v[2], 48), roll(v[3], 96)),
                            jnp.where(lane < 48, roll(v[4], 48), jnp.where(lane < 64, roll(v[1], 64), roll(v[3], 80)))]
                    left -= 8
                elif left >= 3:
                    v = [rcv[k, g, at + j] for j in range(2)]
                    late = [jnp.where(lane < 48, roll(v[0], 48), roll(v[1], 96))]
                    left -= 3
                else:
                    v, late = [rcv[k, g, at]], []
                    left -= 1
                tails += v + [w.astype(BF16) for w in late]
                at += len(v)
            return jnp.concatenate([first, second, jnp.concatenate(tails, axis=0)], axis=1)

        def fit_group(g, carry):
            with jax.named_scope(f'hwait{s}'):
                all_here(rcv.at[pl.ds(1, 7), g, pl.ds(off, SUBSETS[s][3])], hr_sem.at[g, s])
            lhs = jnp.concatenate([jnp.concatenate([half(k, g), half(k + 4, g)], axis=1) for k in range(4)], axis=0)
            t = _dot(jnp.concatenate([lhs, lhs, lhs], axis=1), m_ref[...])
            h2 = hl[0, g, pl.ds(i0, n)].reshape(n * GROUP, QP)
            h3 = hl[1, g, pl.ds(i0, n)].reshape(n * GROUP, QP)
            ca = _dot(jnp.concatenate([h2, h3], axis=0), m_ref[pl.ds(0, QP), :])
            cb = _dot(h2, m_ref[pl.ds(2 * QP, QP), :])
            w = n * GROUP
            for k in range(4):
                _, px, pc = peer(k)
                part = t[k * w:(k + 1) * w]
                if k == 0:
                    part = part + (ca[:w] + (ca[w:] + cb))
                row = pl.multiple_of((px * 2 + pc) * ROWS + g * GROUP, GROUP)
                t_ref[pl.ds(0, n), pl.ds(row, GROUP), :] = part.reshape(n, GROUP, 2 * QP)
            return carry

        with jax.named_scope(f'fit{s}'):
            lax.fori_loop(g0, g1, fit_group, 0)

    def exchange_subset(s):
        n = SUBSETS[s][1]
        step = 4 if n % 4 == 0 else n

        def exchange(i, carry):
            terms = zip(*[_split(t_ref[step * i + j]) for j in range(step)])
            t1, t2, t3 = [jnp.concatenate(v, axis=1) for v in terms]
            both = _dot_nt(jnp.concatenate([t1, t2], axis=0), t2)
            kacc[...] += _dot_nt(t1, t1) + both[L:]
            xacc[...] += both[:L] + _dot_nt(t1, t3)
            return carry

        with jax.named_scope(f'exch{s}'):
            lax.fori_loop(0, n // step, exchange, 0)

    kacc[...] = jnp.zeros_like(kacc)
    xacc[...] = jnp.zeros_like(xacc)
    fit(0, 0, 1)

    with jax.named_scope('gwait'):
        all_here(gr_ref.at[pl.ds(1, 7)], gr_sem)
    for g in range(GROUPS):
        h_send(g, 2)
    gam = jnp.concatenate([ga_ref[...] + gr_ref[1] + gr_ref[2] + gr_ref[3],
                           gr_ref[4] + gr_ref[5] + gr_ref[6] + gr_ref[7]], axis=1)
    gam = jnp.concatenate([gam, jnp.zeros_like(gam)], axis=0)

    def stack(v):
        return jnp.concatenate([t.astype(F32) for t in _split(v)], axis=0).astype(BF16)

    def three(v, dot):
        r1, r2, r3 = dot(v, 0), dot(v[:16], 1), dot(v[:8], 2)
        return r1[:8] + ((r1[8:16] + r2[:8]) + (r1[16:] + (r2[8:] + r3)))

    fitted = three(stack(gam), lambda v, j: _dot(v, m_ref[pl.ds(j * 2 * QP, 2 * QP), :]))
    weights = three(stack(fitted), lambda v, j: _dot(v, m_ref[pl.ds(j * 2 * QP, 2 * QP), pl.ds(0, QP)]))
    wf = jnp.concatenate([t.astype(F32) for t in _split(weights)], axis=0)
    for q in range(4):
        blocks = [jnp.zeros((WPAD * q, QP), F32)] if q else []
        wide = jnp.concatenate(blocks + [wf, jnp.zeros((128 - 24 - WPAD * q, QP), F32)], axis=0)
        wt = wide.T.astype(BF16)
        for j in range(3):
            w_ref[pl.ds((3 * q + j) * QP, QP), :] = wt

    def coulomb(p, carry):
        terms = [t for q in range(4) for t in _split(_padq(b_ref[4 * p + q]))]
        r = _dot(jnp.concatenate(terms, axis=1), w_ref[...]).T
        for q in range(4):
            j_ref[4 * p + q] = r[WPAD * q:WPAD * q + 8] + (r[WPAD * q + 8:WPAD * q + 16] + r[WPAD * q + 16:WPAD * q + 24])
        return carry

    with jax.named_scope('coulomb'):
        lax.fori_loop(0, ROWS // 4, coulomb, 0)
    away = []
    for d in range(DENS):
        jd = j_ref[:, d, :]
        jown[d] = jnp.where(a == 0, jd[:, :96], jd[:, 96:])
        away.append(jnp.where(a == 0, jd[:, 96:], jd[:, :96]))
    jsend[...] = jnp.concatenate(away, axis=1)
    for g in range(GROUPS):
        h_send(g, 3)
    j_copy().start()


    fit(0, 1, GROUPS)
    exchange_subset(0)
    for s in range(1, len(SUBSETS)):
        fit(s, 0, GROUPS)
        exchange_subset(s)

    j_copy().wait_recv()
    theirs = jrecv[...]
    for d in range(DENS):
        jown[d] = 2.0 * (jown[d] + theirs[:, 96 * d:96 * (d + 1)])
    kacc[...] += xacc[...] + xacc[...].T
    for k in (7, 6, 5, 4, 3, 2, 1, 0):
        pa, px, pc = peer(k)
        rows = kacc[pl.ds(pl.multiple_of((px * 2 + pc) * ROWS, 8), ROWS), :]
        part = jnp.where(pa == 0, rows[:, :96], rows[:, 96:])
        if k:
            ksend[k] = part
        else:
            krecv[0] = part
    for k in (7, 6, 5, 4, 3, 2, 1):
        k_copy(k).start()
    with jax.named_scope('kwait'):
        all_here(krecv.at[pl.ds(1, 7)], kr_sem)
    for k in (0, 2, 4, 6):
        pa, px, _ = peer(k)
        d = pa * 2 + px
        out_ref[d] = jown[d] - (krecv[k] + krecv[k + 1])

    all_sent(snd, hs_sem)
    all_sent(gr_ref.at[pl.ds(1, 7)], gs_sem)
    all_sent(ksend.at[pl.ds(1, 7)], ks_sem)
    all_sent(mr, ms_sem)
    j_copy().wait_send()


def solution(mesh):
    def local_fock(ints_blk, metric_blk, orbitals):
        bt = jnp.transpose(ints_blk, (1, 2, 0))
        ct = jnp.transpose(orbitals, (0, 2, 1)).reshape(COLS, L)
        ns = len(SUBSETS)
        dma = pltpu.SemaphoreType.DMA
        return pl.pallas_call(
            kernel,
            out_shape=jax.ShapeDtypeStruct((DENS, ROWS, 96), F32),
            in_specs=[pl.BlockSpec(memory_space=pltpu.HBM)] * 3,
            out_specs=pl.BlockSpec(memory_space=pltpu.VMEM),
            scratch_shapes=[
                pltpu.VMEM((ROWS, L, QL), F32),
                pltpu.VMEM((COLS, L), F32),
                pltpu.VMEM((QL, 2 * QL), F32),
                pltpu.VMEM((3, COLS, L), BF16),
                pltpu.VMEM((L, COLS), F32),
                pltpu.VMEM((ROWS, 8, L), F32),
                pltpu.VMEM((3, GROUP * STRIDE, 128), F32),
                pltpu.VMEM((7, GROUPS, SLOTS, GROUP, 128), BF16),
                pltpu.VMEM((8, GROUPS, SLOTS, GROUP, 128), BF16),
                pltpu.VMEM((2, GROUPS, MINE, GROUP, QP), BF16),
                pltpu.VMEM((6 * QP, 2 * QP), BF16),
                pltpu.VMEM((QL, QP), F32),
                pltpu.VMEM((4, MQ, QP), F32),
                pltpu.VMEM((MAXSUB, L, 2 * QP), F32),
                pltpu.VMEM((12 * QP, 128), BF16),
                pltpu.VMEM((8, QP), F32),
                pltpu.VMEM((DENS, QP), F32),
                pltpu.VMEM((8, DENS, QP), F32),
                pltpu.VMEM((ROWS, 8, L), F32),
                pltpu.VMEM((DENS, ROWS, 96), F32),
                pltpu.VMEM((ROWS, DENS * 96), F32),
                pltpu.VMEM((ROWS, DENS * 96), F32),
                pltpu.VMEM((L, L), F32),
                pltpu.VMEM((L, L), F32),
                pltpu.VMEM((8, ROWS, 96), F32),
                pltpu.VMEM((8, ROWS, 96), F32),
                dma((4,)), dma((2,)), dma, dma((GROUPS, ns)), dma, dma((3,)),
                dma, dma, dma, dma, dma, dma,
            ],
            compiler_params=pltpu.CompilerParams(collective_id=0, has_side_effects=True, vmem_limit_bytes=56_360_000),
            cost_estimate=pl.CostEstimate(flops=25_000_000_000, bytes_accessed=16_000_000, transcendentals=0),
        )(bt, ct, metric_blk)

    return jax.shard_map(local_fock, mesh=mesh, in_specs=(P(('sys', 'aux'), 'orb', None), P(('sys', 'aux'), None), P('sys', None, None)), out_specs=P('sys', 'orb', 'aux'), check_vma=False)
```
